32 devices in a mesh: dp: 2 (over x), tp: 4 (over z), cp: 4 (over y, core).
Axes of the slice: x: 2, y: 2, z: 4, core: 2. Of those that a mesh axis runs over, the one named last changes fastest.
Arguments:
- x_chunk: bfloat16 [16, 512, 2048], P('dp', 'cp'), parts along dimension 0
- w_query: bfloat16 [2048, 2048], P(None, 'tp')
- w_key: bfloat16 [2048, 2048], P(None, 'tp')
- w_value: bfloat16 [2048, 2048], P(None, 'tp')
- w_out: bfloat16 [2048, 2048], P('tp')
- q_gain: bfloat16 [2048], P('tp')
- k_gain: bfloat16 [2048], P('tp')
- post_gain: bfloat16 [2048], replicated
- cache_k: bfloat16 [16, 8192, 16, 128], P('dp', 'cp', 'tp'), parts along dimension 0
- cache_v: bfloat16 [16, 8192, 16, 128], P('dp', 'cp', 'tp'), parts along dimension 0
- prefix_len: int32 [16], P('dp'), parts along dimension 0
Outputs:
- output 1: bfloat16 [16, 512, 2048], P('dp', 'cp'), parts along dimension 0
- output 2: bfloat16 [16, 512, 16, 128], P('dp', 'cp', 'tp'), parts along dimension 0
- output 3: bfloat16 [16, 512, 16, 128], P('dp', 'cp', 'tp'), parts along dimension 0
There are 2 independent parts. The reference program is written for one: setup_inputs(seed, part) draws one part's arguments, and reference() takes and returns one part's arrays. A program takes and returns all parts, laid end to end along the dimension named above; an argument that names none is the same for every part.
All inputs are finite; a program needn't handle non-finite values.
Results may differ from the reference program's by a relative error of at most 0.00736104.
Values are sent between devices in bfloat16 or wider.
A program may use at most 1 GiB of HBM per device.

```python
import jax
import jax.numpy as jnp
from jax import lax

BATCH_ROWS = 8
CHUNK_LEN = 512
CACHE_LEN = 8192
MODEL_DIM = 2048
Q_HEADS = 16
KV_HEADS = 16
HEAD_DIM = 128
QUERY_BLOCK = min(CHUNK_LEN, 16)
ROPE_BASE = 500000.0
NORM_EPS = 1e-6


def head_scales(rng_key, n_heads, trend_slope):
    trend_pos = jnp.arange(n_heads, dtype=jnp.float32) * (2.0 / max(n_heads - 1, 1)) - 1.0
    noise_val = jax.random.normal(rng_key, (n_heads,), jnp.float32)
    return jnp.exp(trend_slope * trend_pos + 0.2 * noise_val)


def draw_prefix(rng_key):
    key_order, key_len = jax.random.split(rng_key)
    row_order = jax.random.permutation(key_order, BATCH_ROWS)
    lengths = jax.random.randint(key_len, (BATCH_ROWS,), CACHE_LEN // 2, CACHE_LEN + 1)
    lengths = jnp.where(row_order == 0, CACHE_LEN, jnp.where(row_order == 1, CACHE_LEN // 2, lengths))
    return lengths.astype(jnp.int32)


def setup_inputs(seed: int = 0, part: int = 0) -> dict:
    shared_keys = jax.random.split(jax.random.key(seed), 9)
    own_keys = jax.random.split(jax.random.fold_in(jax.random.key(seed + 1), part), 4)
    q_width = Q_HEADS * HEAD_DIM
    kv_width = KV_HEADS * HEAD_DIM
    q_cols = jnp.repeat(head_scales(shared_keys[0], Q_HEADS, 0.5), HEAD_DIM)
    k_cols = jnp.repeat(head_scales(shared_keys[1], KV_HEADS, 0.5), HEAD_DIM)
    w_query = jax.random.normal(shared_keys[2], (MODEL_DIM, q_width), jnp.float32) * (MODEL_DIM ** -0.5) * q_cols[None, :]
    w_key = jax.random.normal(shared_keys[3], (MODEL_DIM, kv_width), jnp.float32) * (MODEL_DIM ** -0.5) * k_cols[None, :]
    w_value = jax.random.normal(shared_keys[4], (MODEL_DIM, kv_width), jnp.float32) * (MODEL_DIM ** -0.5)
    w_out = jax.random.normal(shared_keys[5], (q_width, MODEL_DIM), jnp.float32) * (q_width ** -0.5)
    q_gain = 1.0 + 0.25 * jax.random.normal(shared_keys[6], (q_width,), jnp.float32)
    k_gain = 1.0 + 0.25 * jax.random.normal(shared_keys[7], (kv_width,), jnp.float32)
    post_gain = 1.0 + 0.3 * jax.random.normal(shared_keys[8], (MODEL_DIM,), jnp.float32)
    prefix_len = draw_prefix(own_keys[0])
    x_chunk = jax.random.normal(own_keys[1], (BATCH_ROWS, CHUNK_LEN, MODEL_DIM), jnp.float32)
    stale_mask = jnp.arange(CACHE_LEN)[None, :] >= prefix_len[:, None]
    slot_scale = jnp.where(stale_mask, 3.0, 1.0)[:, :, None, None]
    cache_k = 0.8 * jax.random.normal(own_keys[2], (BATCH_ROWS, CACHE_LEN, KV_HEADS, HEAD_DIM), jnp.float32) * slot_scale
    cache_v = jax.random.normal(own_keys[3], (BATCH_ROWS, CACHE_LEN, KV_HEADS, HEAD_DIM), jnp.float32) * slot_scale
    return {
        'x_chunk': x_chunk.astype(jnp.bfloat16),
        'w_query': w_query.astype(jnp.bfloat16),
        'w_key': w_key.astype(jnp.bfloat16),
        'w_value': w_value.astype(jnp.bfloat16),
        'w_out': w_out.astype(jnp.bfloat16),
        'q_gain': q_gain.astype(jnp.bfloat16),
        'k_gain': k_gain.astype(jnp.bfloat16),
        'post_gain': post_gain.astype(jnp.bfloat16),
        'cache_k': cache_k.astype(jnp.bfloat16),
        'cache_v': cache_v.astype(jnp.bfloat16),
        'prefix_len': prefix_len,
    }


def rms_norm(raw_vals, gain_vec):
    mean_sq = jnp.mean(raw_vals * raw_vals, axis=-1, keepdims=True)
    return raw_vals * lax.rsqrt(mean_sq + NORM_EPS) * gain_vec.astype(jnp.float32)


def rope_apply(head_vals, positions):
    half_dim = HEAD_DIM // 2
    inv_freq = ROPE_BASE ** (-(jnp.arange(half_dim, dtype=jnp.float32) * 2.0 / HEAD_DIM))
    angles = positions.astype(jnp.float32)[..., None] * inv_freq
    cos_tab = jnp.cos(angles)[..., None, :]
    sin_tab = jnp.sin(angles)[..., None, :]
    first_half = head_vals[..., :half_dim]
    second_half = head_vals[..., half_dim:]
    return jnp.concatenate([first_half * cos_tab - second_half * sin_tab, second_half * cos_tab + first_half * sin_tab], axis=-1)


def reference(x_chunk, w_query, w_key, w_value, w_out, q_gain, k_gain, post_gain, cache_k, cache_v, prefix_len):
    groups = Q_HEADS // KV_HEADS
    tokens = x_chunk.reshape(BATCH_ROWS * CHUNK_LEN, MODEL_DIM)
    q_raw = jnp.dot(tokens, w_query, preferred_element_type=jnp.float32)
    k_raw = jnp.dot(tokens, w_key, preferred_element_type=jnp.float32)
    v_raw = jnp.dot(tokens, w_value, preferred_element_type=jnp.float32)
    positions = prefix_len[:, None] + jnp.arange(CHUNK_LEN, dtype=jnp.int32)[None, :]
    q_rot = rope_apply(rms_norm(q_raw, q_gain).reshape(BATCH_ROWS, CHUNK_LEN, Q_HEADS, HEAD_DIM), positions)
    k_rot = rope_apply(rms_norm(k_raw, k_gain).reshape(BATCH_ROWS, CHUNK_LEN, KV_HEADS, HEAD_DIM), positions)
    q_new = q_rot.astype(jnp.bfloat16).reshape(BATCH_ROWS, CHUNK_LEN, KV_HEADS, groups, HEAD_DIM)
    chunk_k = k_rot.astype(jnp.bfloat16)
    chunk_v = v_raw.astype(jnp.bfloat16).reshape(BATCH_ROWS, CHUNK_LEN, KV_HEADS, HEAD_DIM)
    key_index = jnp.arange(CACHE_LEN + CHUNK_LEN)
    score_scale = HEAD_DIM ** -0.5

    def row_attention(row_in):
        q_row, k_row, v_row, ck_row, cv_row, valid_len = row_in
        all_keys = jnp.concatenate([ck_row, k_row], axis=0).astype(jnp.float32)
        all_values = jnp.concatenate([cv_row, v_row], axis=0).astype(jnp.float32)
        q_blocks = q_row.reshape(CHUNK_LEN // QUERY_BLOCK, QUERY_BLOCK, KV_HEADS, groups, HEAD_DIM).astype(jnp.float32)

        def block_attention(block_in):
            q_blk, block_id = block_in
            q_index = block_id * QUERY_BLOCK + jnp.arange(QUERY_BLOCK)
            allowed = jnp.where(key_index[None, :] < CACHE_LEN, key_index[None, :] < valid_len, key_index[None, :] - CACHE_LEN <= q_index[:, None])
            scores = jnp.einsum('qkgd,tkd->qkgt', q_blk, all_keys) * score_scale
            scores = jnp.where(allowed[:, None, None, :], scores, -jnp.inf)
            probs_f = jax.nn.softmax(scores, axis=-1)
            return jnp.einsum('qkgt,tkd->qkgd', probs_f, all_values)

        blocks = lax.map(block_attention, (q_blocks, jnp.arange(CHUNK_LEN // QUERY_BLOCK)))
        return blocks.reshape(CHUNK_LEN, Q_HEADS * HEAD_DIM)

    attn_out = lax.map(row_attention, (q_new, chunk_k, chunk_v, cache_k, cache_v, prefix_len))
    attn_out = attn_out.astype(jnp.bfloat16).reshape(BATCH_ROWS * CHUNK_LEN, Q_HEADS * HEAD_DIM)
    mixed_sum = jnp.dot(attn_out, w_out, preferred_element_type=jnp.float32)
    result = x_chunk.astype(jnp.float32) + rms_norm(mixed_sum, post_gain).reshape(BATCH_ROWS, CHUNK_LEN, MODEL_DIM)
    return result.astype(jnp.bfloat16), chunk_k, chunk_v
```

```python
import functools
import jax
import jax.numpy as jnp
from jax import lax
from jax.experimental import pallas as pl
from jax.experimental.pallas import tpu as pltpu
from jax.sharding import PartitionSpec as P

NORM_EPS = 1e-6
ROPE_BASE = 500000.0
MASK_VALUE = -1e30
LOG2E = 1.4426950408889634


def rope_apply(head_vals, positions):
    head_dim = head_vals.shape[-1]
    half_dim = head_dim // 2
    inv_freq = ROPE_BASE ** (-(jnp.arange(half_dim, dtype=jnp.float32) * 2.0 / head_dim))
    angles = positions.astype(jnp.float32)[..., None] * inv_freq
    cos_tab = jnp.cos(angles)[..., None, :]
    sin_tab = jnp.sin(angles)[..., None, :]
    first_half = head_vals[..., :half_dim]
    second_half = head_vals[..., half_dim:]
    return jnp.concatenate([first_half * cos_tab - second_half * sin_tab, second_half * cos_tab + first_half * sin_tab], axis=-1)


def split_heads(raw_ref, wide_ref, out_ref, heads, rows):
    step = wide_ref.shape[0]
    per = step // heads

    def body(i, _):
        wide_ref[...] = raw_ref[pl.ds(i * step, step), :].astype(jnp.float32)
        for h in range(heads):
            out_ref[h, pl.ds(i * per, per), :] = wide_ref[pl.ds(h, per, stride=heads), :].astype(jnp.bfloat16)
        return 0

    lax.fori_loop(0, rows // step, body, 0)


def attend_head(h, q, k_ref, v_ref, kc, vc, s_ref, limit, chunk_ok, tile):
    n_q = q.shape[0]
    n_t = k_ref.shape[1] // tile
    lane = lax.broadcasted_iota(jnp.int32, (1, tile), 1)
    nt = (((1,), (1,)), ((), ()))
    s_c = lax.dot_general(q, kc, nt, preferred_element_type=jnp.float32)
    s_c = jnp.where(chunk_ok, s_c, MASK_VALUE)
    mx = s_c
    for j in range(n_t):
        s = lax.dot_general(q, k_ref[h, j * tile:(j + 1) * tile, :], nt, preferred_element_type=jnp.float32)
        s = jnp.where(lane + j * tile < limit, s, MASK_VALUE)
        s_ref[:, j * tile:(j + 1) * tile] = s
        for u in range(tile // 128):
            mx = jnp.maximum(mx, s[:, u * 128:(u + 1) * 128])
    c = (128 ** -0.5) * LOG2E
    m = jnp.max(mx, axis=1, keepdims=True)
    p = jnp.exp2((s_c - m) * c)
    l = p
    acc = jnp.dot(p.astype(jnp.bfloat16), vc, preferred_element_type=jnp.float32)
    for j in range(n_t):
        p = jnp.exp2((s_ref[:, j * tile:(j + 1) * tile] - m) * c)
        for u in range(tile // 128):
            l = l + p[:, u * 128:(u + 1) * 128]
        acc = acc + jnp.dot(p.astype(jnp.bfloat16), v_ref[h, j * tile:(j + 1) * tile, :], preferred_element_type=jnp.float32)
    l = jnp.sum(l, axis=1, keepdims=True)
    return acc * (1.0 / l), m * c + jnp.log2(l)


def attn_kernel(pre_ref, q_ref, kn_ref, vn_ref, ck_ref, cv_ref, o_ref, lse_ref, wide, k_scr, v_scr, s_scr):
    b = pl.program_id(0)
    cp = lax.axis_index('cp')
    heads = k_scr.shape[0]
    slots = k_scr.shape[1]
    limit = pre_ref[b] - cp * slots
    split_heads(ck_ref.at[0], wide, k_scr, heads, slots * heads)
    split_heads(cv_ref.at[0], wide, v_scr, heads, slots * heads)
    n_q = q_ref.shape[1]
    n_k = kn_ref.shape[1]
    qi = lax.broadcasted_iota(jnp.int32, (n_q, n_k), 0)
    ki = lax.broadcasted_iota(jnp.int32, (n_q, n_k), 1)
    chunk_ok = ki + cp * n_k <= qi
    lane = lax.broadcasted_iota(jnp.int32, (n_q, 128), 1)

    lse_ref[0] = jnp.zeros(lse_ref.shape[1:], jnp.float32)

    def head(h, _):
        col = pl.ds(pl.multiple_of(h * 128, 128), 128)
        o, lse = attend_head(h, q_ref[0, :, col], k_scr, v_scr, kn_ref[0, :, col], vn_ref[0, :, col], s_scr, limit, chunk_ok, 256)
        o_ref[0, :, col] = o.astype(jnp.bfloat16)
        lse_ref[0] = jnp.where(lane == h, lse, lse_ref[0])
        return 0

    lax.fori_loop(0, heads, head, 0)


def attention(prefix_len, q_all, k_new, v_new, cache_k, cache_v):
    rows, n_q, width = q_all.shape
    slots, heads = cache_k.shape[1], cache_k.shape[2]
    ck = cache_k.reshape(rows, slots * heads, 128)
    cv = cache_v.reshape(rows, slots * heads, 128)
    blk = lambda *s: pl.BlockSpec((1,) + s, lambda b, pre: (b, 0, 0))
    spec = pltpu.PrefetchScalarGridSpec(
        num_scalar_prefetch=1, grid=(rows,),
        in_specs=[blk(n_q, width), blk(k_new.shape[1], width), blk(k_new.shape[1], width), blk(slots * heads, 128), blk(slots * heads, 128)],
        out_specs=[blk(n_q, width), blk(n_q, 128)],
        scratch_shapes=[pltpu.VMEM((1024, 128), jnp.float32), pltpu.VMEM((heads, slots, 128), jnp.bfloat16), pltpu.VMEM((heads, slots, 128), jnp.bfloat16), pltpu.VMEM((n_q, slots), jnp.float32)])
    return pl.pallas_call(
        attn_kernel, grid_spec=spec,
        out_shape=[jax.ShapeDtypeStruct((rows, n_q, width), jnp.bfloat16), jax.ShapeDtypeStruct((rows, n_q, 128), jnp.float32)],
        compiler_params=pltpu.CompilerParams(dimension_semantics=("arbitrary",), vmem_limit_bytes=56 << 20),
        cost_estimate=pl.CostEstimate(flops=4 * rows * n_q * slots * width, bytes_accessed=4 * rows * slots * width, transcendentals=rows * n_q * slots * heads),
        name="attn")(prefix_len, q_all, k_new, v_new, ck, cv)


def solution(mesh):
    cp_size = mesh.shape['cp']
    tp_size = mesh.shape['tp']

    def local_step(x_chunk, w_query, w_key, w_value, w_out, q_gain, k_gain, post_gain, cache_k, cache_v, prefix_len):
        batch_rows, chunk_dev, model_dim = x_chunk.shape
        heads = cache_k.shape[2]
        head_dim = cache_k.shape[3]
        width = heads * head_dim
        cp_index = lax.axis_index('cp')
        tokens = x_chunk.reshape(batch_rows * chunk_dev, model_dim)
        q_raw = jnp.dot(tokens, w_query, preferred_element_type=jnp.float32)
        k_raw = jnp.dot(tokens, w_key, preferred_element_type=jnp.float32)
        v_raw = jnp.dot(tokens, w_value, preferred_element_type=jnp.float32)
        square_sums = lax.psum(jnp.stack([jnp.sum(q_raw * q_raw, axis=-1), jnp.sum(k_raw * k_raw, axis=-1)]), 'tp')
        q_inv = lax.rsqrt(square_sums[0] / (width * tp_size) + NORM_EPS)
        k_inv = lax.rsqrt(square_sums[1] / (width * tp_size) + NORM_EPS)
        q_norm = (q_raw * q_inv[:, None] * q_gain.astype(jnp.float32)).reshape(batch_rows, chunk_dev, heads, head_dim)
        k_norm = (k_raw * k_inv[:, None] * k_gain.astype(jnp.float32)).reshape(batch_rows, chunk_dev, heads, head_dim)
        positions = prefix_len[:, None] + cp_index * chunk_dev + jnp.arange(chunk_dev, dtype=jnp.int32)[None, :]
        q_new = rope_apply(q_norm, positions).astype(jnp.bfloat16).reshape(batch_rows, chunk_dev, width)
        k_new = rope_apply(k_norm, positions).astype(jnp.bfloat16).reshape(batch_rows, chunk_dev, width)
        v_new = v_raw.astype(jnp.bfloat16).reshape(batch_rows, chunk_dev, width)
        q_all = lax.all_gather(q_new, 'cp', axis=1, tiled=True)
        o_part, lse = attention(prefix_len, q_all, k_new, v_new, cache_k, cache_v)
        o_part = lax.all_to_all(o_part.reshape(batch_rows, cp_size, chunk_dev, width), 'cp', 1, 1)
        lse = lax.all_to_all(lse[:, :, :heads].reshape(batch_rows, cp_size, chunk_dev, heads), 'cp', 1, 1)
        lse = lse - jnp.max(lse, axis=1, keepdims=True)
        wt = jnp.exp2(lse)
        wt = wt / jnp.sum(wt, axis=1, keepdims=True)
        o = jnp.sum(o_part.astype(jnp.float32).reshape(batch_rows, cp_size, chunk_dev, heads, head_dim) * wt[..., None], axis=1)
        attn_out = o.astype(jnp.bfloat16).reshape(batch_rows * chunk_dev, width)
        mixed = jnp.dot(attn_out, w_out, preferred_element_type=jnp.float32).astype(jnp.bfloat16)
        mixed = lax.all_to_all(mixed.reshape(tp_size, -1, model_dim), 'tp', 0, 0)
        mixed = jnp.sum(mixed.astype(jnp.float32), axis=0)
        normed = mixed * lax.rsqrt(jnp.mean(mixed * mixed, axis=-1, keepdims=True) + NORM_EPS) * post_gain.astype(jnp.float32)
        tp_index = lax.axis_index('tp')
        n = tokens.shape[0] // tp_size
        mine = lax.dynamic_slice_in_dim(tokens, tp_index * n, n, axis=0)
        out = (mine.astype(jnp.float32) + normed).astype(jnp.bfloat16)
        block_out = lax.all_gather(out, 'tp', axis=0, tiled=True).reshape(x_chunk.shape)
        return block_out, k_new.reshape(batch_rows, chunk_dev, heads, head_dim), v_new.reshape(batch_rows, chunk_dev, heads, head_dim)

    x_spec = P('dp', 'cp', None)
    head_spec = P('dp', 'cp', 'tp', None)
    in_specs = (x_spec, P(None, 'tp'), P(None, 'tp'), P(None, 'tp'), P('tp', None), P('tp'), P('tp'), P(None), head_spec, head_spec, P('dp'))
    out_specs = (x_spec, head_spec, head_spec)
    return jax.shard_map(local_step, mesh=mesh, in_specs=in_specs, out_specs=out_specs, check_vma=False)
```

```python
import functools
import jax
import jax.numpy as jnp
from jax import lax
from jax.experimental import pallas as pl
from jax.experimental.pallas import tpu as pltpu
from jax.sharding import PartitionSpec as P

NORM_EPS = 1e-6
ROPE_BASE = 500000.0
MASK_VALUE = -1e30
LOG2E = 1.4426950408889634
MESH = pl.DeviceIdType.MESH
NT = (((1,), (1,)), ((), ()))
F32 = jnp.float32
BF16 = jnp.bfloat16


def split_heads(raw_ref, wide_ref, out_ref, heads, rows):
    step = wide_ref.shape[0]
    per = step // heads

    def body(i, _):
        wide_ref[...] = raw_ref[pl.ds(i * step, step), :].astype(F32)
        for h in range(heads):
            out_ref[h, pl.ds(i * per, per), :] = wide_ref[pl.ds(h, per, stride=heads), :].astype(BF16)
        return 0

    lax.fori_loop(0, rows // step, body, 0)


def attend_head(h, q, k_ref, v_ref, kc, vc, s_ref, limit, bias, tile):
    n_t = k_ref.shape[1] // tile
    lane = lax.broadcasted_iota(jnp.int32, (1, tile), 1)
    s_c = lax.dot_general(q, kc, NT, preferred_element_type=F32)
    s_c = jnp.where(bias >= 0, s_c, MASK_VALUE)
    mx = s_c
    for j in range(n_t):
        s = lax.dot_general(q, k_ref[h, j * tile:(j + 1) * tile, :], NT, preferred_element_type=F32)
        s = jnp.where(lane + j * tile < limit, s, MASK_VALUE)
        s_ref[:, j * tile:(j + 1) * tile] = s
        for u in range(tile // 128):
            mx = jnp.maximum(mx, s[:, u * 128:(u + 1) * 128])
    c = (128 ** -0.5) * LOG2E
    m = jnp.max(mx, axis=1, keepdims=True)
    p = jnp.exp2((s_c - m) * c)
    l = p
    acc = jnp.dot(p.astype(BF16), vc, preferred_element_type=F32)
    for j in range(n_t):
        p = jnp.exp2((s_ref[:, j * tile:(j + 1) * tile] - m) * c)
        for u in range(tile // 128):
            l = l + p[:, u * 128:(u + 1) * 128]
        acc = acc + jnp.dot(p.astype(BF16), v_ref[h, j * tile:(j + 1) * tile, :], preferred_element_type=F32)
    l = jnp.sum(l, axis=1, keepdims=True)
    return acc * (1.0 / l), m * c + jnp.log2(l)


def step_kernel(n_tp, pre_ref, x_hbm, wq_hbm, wk_hbm, wv_hbm, wo_hbm, qg_ref, kg_ref, pg_ref, cos_ref, sin_ref, ck_hbm, cv_hbm,
                out_hbm, ok_hbm, ov_hbm,
                x_v, wqkv, wf, q_buf, kn, vn, rA, rB, rC, lA, lB, lC, c_o, c_l, l_buf, o_all, st,
                raw, wide, k_scr, v_scr, s_scr, bias, lse_scr,
                in_sem, kv_sem, out_sem, st_s, st_r, q_s, q_r, p_s, p_r, z_s, z_r, w_s, w_r):
    rows, toks, model = x_v.shape
    heads, slots = k_scr.shape[0], k_scr.shape[1]
    width = heads * 128
    groups = rows // 2
    gt = 2 * toks
    dp, z, me = lax.axis_index('dp'), lax.axis_index('tp'), lax.axis_index('cp')
    partner = me + 1 - 2 * (me % 2)
    counter = (me + 2) % 4
    diag = 3 - me
    last = n_tp - 1
    piece = wo_hbm.shape[0] // 8

    def remote(src, dst, ss, rs, **dev):
        return pltpu.make_async_remote_copy(src_ref=src, dst_ref=dst, send_sem=ss, recv_sem=rs, device_id=dev, device_id_type=MESH)

    loads = [pltpu.make_async_copy(x_hbm, x_v, in_sem.at[0])]
    for i, w in enumerate((wq_hbm, wk_hbm, wv_hbm)):
        loads.append(pltpu.make_async_copy(w, wqkv.at[i], in_sem.at[1 + i]))
    js = pl.ds(pl.multiple_of((dp * 4 + me) * piece, piece), piece)
    w_local = pltpu.make_async_copy(wo_hbm.at[js, :], wf.at[z, js, :], in_sem.at[4])
    w_local.start()
    for cpy in loads:
        cpy.start()

    def kv_copies(b):
        par = b % 2
        return (pltpu.make_async_copy(ck_hbm.at[b], raw.at[par, 0], kv_sem.at[par, 0]),
                pltpu.make_async_copy(cv_hbm.at[b], raw.at[par, 1], kv_sem.at[par, 1]))

    for cpy in kv_copies(0):
        cpy.start()

    barrier = pltpu.get_barrier_semaphore()
    for i in range(1, n_tp):
        pl.semaphore_signal(barrier, inc=1, device_id={'tp': (z + i) % n_tp}, device_id_type=MESH)
    pl.semaphore_signal(barrier, inc=1, device_id={'cp': partner}, device_id_type=MESH)
    pl.semaphore_signal(barrier, inc=1, device_id={'cp': counter}, device_id_type=MESH)
    pl.semaphore_signal(barrier, inc=1, device_id={'dp': 1 - dp}, device_id_type=MESH)
    pl.semaphore_wait(barrier, n_tp + 2)

    def hop(buf, send, recv, k, wait_only=False, start=True):
        if k > 1:
            @pl.when(z - (k - 1) >= 0)
            def _():
                remote(buf(z - (k - 1)), buf(z - (k - 1)), send(0, k - 2), recv(0, k - 2), tp=z).wait_recv()

            @pl.when(z + (k - 1) <= last)
            def _():
                remote(buf(z + (k - 1)), buf(z + (k - 1)), send(1, k - 2), recv(1, k - 2), tp=z).wait_recv()
        if k <= last:
            @pl.when((z - (k - 1) >= 0) & (z < last))
            def _():
                remote(buf(z - (k - 1)), buf(z - (k - 1)), send(0, k - 1), recv(0, k - 1), tp=z + 1).start()

            @pl.when((z + (k - 1) <= last) & (z > 0))
            def _():
                remote(buf(z + (k - 1)), buf(z + (k - 1)), send(1, k - 1), recv(1, k - 1), tp=z - 1).start()

    def hop_sent(buf, send, recv):
        for k in range(1, last + 1):
            @pl.when((z - (k - 1) >= 0) & (z < last))
            def _():
                remote(buf(z - (k - 1)), buf(z - (k - 1)), send(0, k - 1), recv(0, k - 1), tp=z).wait_send()

            @pl.when((z + (k - 1) <= last) & (z > 0))
            def _():
                remote(buf(z + (k - 1)), buf(z + (k - 1)), send(1, k - 1), recv(1, k - 1), tp=z).wait_send()

    def w_hop(k):
        hop(lambda o: wf.at[o, js, :], lambda d, i: w_s.at[d * last + i], lambda d, i: w_r.at[d * last + i], k)

    def o_hop(b, k):
        hop(lambda o: o_all.at[o, b], lambda d, i: z_s.at[b, d * last + i], lambda d, i: z_r.at[b, d * last + i], k)

    w_local.wait()
    w_hop(1)

    qi = lax.broadcasted_iota(jnp.int32, (toks, toks), 0)
    ki = lax.broadcasted_iota(jnp.int32, (toks, toks), 1)
    for s, blk in enumerate((me, partner, counter, diag)):
        bias[s * toks:(s + 1) * toks, :] = jnp.where(ki - qi <= (blk - me) * toks, 0.0, -1.0)
    lse_scr[...] = jnp.zeros(lse_scr.shape, F32)

    for cpy in loads:
        cpy.wait()

    def st_copy(g, i):
        return remote(st.at[g, 0], st.at[g, i], st_s.at[g, i - 1], st_r.at[g, i - 1], tp=(z + i) % n_tp)

    def q_copy(b, i):
        src = q_buf.at[b, pl.ds(0 if i < 2 else 2 * toks, toks), :]
        dst = q_buf.at[b, pl.ds((i + 1) * toks, toks), :]
        return remote(src, dst, q_s.at[b, i], q_r.at[b, i], cp=counter if i == 1 else partner)

    def project(g):
        xg = x_v[pl.ds(2 * g, 2)].reshape(gt, model)
        cols = pl.ds(pl.multiple_of(g * width, width), width)
        q = jnp.dot(xg, wqkv[0], preferred_element_type=F32)
        s_scr[0:gt, cols] = q
        k = jnp.dot(xg, wqkv[1], preferred_element_type=F32)
        s_scr[gt:2 * gt, cols] = k
        lane = lax.broadcasted_iota(jnp.int32, (gt, 128), 1)
        sq = jnp.sum(q * q, axis=1, keepdims=True)
        sk = jnp.sum(k * k, axis=1, keepdims=True)
        sums = jnp.where(lane == 0, sq, jnp.where(lane == 1, sk, 0.0))
        st[g, 0] = jnp.transpose(sums)[0:8, :]
        v = jnp.dot(xg, wqkv[2], preferred_element_type=F32)
        for i in range(1, n_tp):
            st_copy(g, i).start()
        vn[pl.ds(2 * g, 2)] = v.astype(BF16).reshape(2, toks, width)

    def normalize(g):
        for i in range(1, n_tp):
            st_copy(g, i).wait_recv()
        tot = st[g, 0]
        for i in range(1, n_tp):
            tot = tot + st[g, i]
        inv = jnp.transpose(lax.rsqrt(tot / (width * n_tp) + NORM_EPS))
        for t, (gain, base) in enumerate(((qg_ref, 0), (kg_ref, gt))):
            for h in range(heads):
                u = s_scr[base:base + gt, pl.ds(pl.multiple_of(g * width + h * 128, 128), 128)]
                u = u * inv[:, t:t + 1] * gain[0:1, h * 128:(h + 1) * 128].astype(F32)
                cos = cos_ref[pl.ds(2 * g, 2)].reshape(gt, 128)
                sin = sin_ref[pl.ds(2 * g, 2)].reshape(gt, 128)
                u = (u * cos + pltpu.roll(u, 64, 1) * sin).astype(BF16).reshape(2, toks, 128)
                if t == 0:
                    q_buf[pl.ds(2 * g, 2), 0:toks, h * 128:(h + 1) * 128] = u
                else:
                    kn[pl.ds(2 * g, 2), :, h * 128:(h + 1) * 128] = u
        for r in range(2):
            q_copy(2 * g + r, 0).start()
            q_copy(2 * g + r, 1).start()

    def front(g, _):
        @pl.when(g < groups)
        def _():
            project(g)

        @pl.when(g == 1)
        def _():
            w_hop(2)

        @pl.when(g == 2)
        def _():
            w_hop(3)

        @pl.when(g > 0)
        def _():
            normalize(g - 1)
        return 0

    lax.fori_loop(0, groups + 1, front, 0)

    outs = (pltpu.make_async_copy(kn, ok_hbm, out_sem.at[groups]), pltpu.make_async_copy(vn, ov_hbm, out_sem.at[groups + 1]))
    for cpy in outs:
        cpy.start()

    nw = 2 * last

    def wslice(d, c):
        return wf.at[:, pl.ds(pl.multiple_of((d * 4 + c) * piece, piece), piece), :]

    def w_copy(i):
        ref = (wslice(dp, me), wslice(dp, me), wslice(dp, me), wslice(dp, counter), wslice(dp, counter), wslice(1 - dp, me), wslice(1 - dp, counter))[i]
        dev = ({'cp': counter}, {'dp': 1 - dp}, {'cp': partner}, {'dp': 1 - dp}, {'cp': partner}, {'cp': partner}, {'cp': partner})[i]
        return remote(ref, ref, w_s.at[nw + i], w_r.at[nw + i], **dev)

    w_hop(4)
    for i in range(3):
        w_copy(i).start()

    def forward_q(b):
        q_copy(b, 1).wait_recv()
        q_copy(b, 2).start()

    forward_q(0)

    def p_copy(b, i):
        if i < 4:
            s = 1 if i < 2 else 3
            src = (q_buf.at[b, pl.ds(s * toks, toks), :], l_buf.at[b, :, pl.ds(s * toks, toks)])[i % 2]
        else:
            src = (c_o.at[b], c_l.at[b])[i % 2]
        dst = (rA.at[b], lA.at[b], rB.at[b], lB.at[b], rC.at[b], lC.at[b])[i]
        return remote(src, dst, p_s.at[b, i], p_r.at[b, i], cp=partner if i < 4 else counter)

    def blend(parts, dst):
        top = functools.reduce(jnp.maximum, [e for _, e in parts])
        ws = [jnp.exp2(e - top) for _, e in parts]
        den = functools.reduce(jnp.add, ws)
        cols = [jnp.transpose(w / den) for w in ws]
        for h in range(heads):
            hs = slice(h * 128, (h + 1) * 128)
            acc = functools.reduce(jnp.add, [c[:, h:h + 1] * v[:, hs].astype(F32) for c, (v, _) in zip(cols, parts)])
            dst[:, hs] = acc.astype(BF16)
        return top + jnp.log2(den)

    def precombine(b):
        p_copy(b, 2).wait_recv()
        p_copy(b, 3).wait_recv()
        c_l[b] = blend([(q_buf.at[b, pl.ds(2 * toks, toks), :], l_buf[b, :, 2 * toks:3 * toks]), (rB.at[b], lB[b])], c_o.at[b])
        p_copy(b, 4).start()
        p_copy(b, 5).start()

    def finish(b):
        for i in (0, 1, 4, 5):
            p_copy(b, i).wait_recv()
        blend([(q_buf.at[b, pl.ds(0, toks), :], l_buf[b, :, 0:toks]), (rA.at[b], lA[b]), (rC.at[b], lC[b])], o_all.at[z, b])
        o_hop(b, 1)

    def out_copy(g):
        return pltpu.make_async_copy(x_v.at[pl.ds(2 * g, 2)], out_hbm.at[pl.ds(2 * g, 2)], out_sem.at[g])

    def project_out(g):
        o_hop(2 * g, 4)
        o_hop(2 * g + 1, 4)

        def chunk(n, ss):
            cols = pl.ds(pl.multiple_of(n * 512, 512), 512)
            y = None
            for t in range(n_tp):
                d = jnp.dot(o_all[t, pl.ds(2 * g, 2)].reshape(gt, width), wf[t, :, cols], preferred_element_type=F32)
                y = d if y is None else y + d
            s_scr[0:gt, cols] = y
            return ss + jnp.sum(y * y, axis=1, keepdims=True)

        ss = lax.fori_loop(0, model // 512, chunk, jnp.zeros((gt, 1), F32))
        inv = lax.rsqrt(ss / model + NORM_EPS)
        for n in range(model // 512):
            cols = slice(n * 512, (n + 1) * 512)
            y = s_scr[0:gt, cols] * inv * pg_ref[0:1, cols].astype(F32)
            y = x_v[pl.ds(2 * g, 2), :, cols].reshape(gt, 512).astype(F32) + y
            x_v[pl.ds(2 * g, 2), :, cols] = y.astype(BF16).reshape(2, toks, 512)
        out_copy(g).start()

    head_lane = lax.broadcasted_iota(jnp.int32, lse_scr.shape, 1)

    def row(b, _):
        @pl.when(b < rows)
        def _():
            for cpy in kv_copies(b):
                cpy.wait()

            @pl.when(b + 1 < rows)
            def _():
                for cpy in kv_copies(b + 1):
                    cpy.start()
                forward_q(b + 1)

            split_heads(raw.at[b % 2, 0], wide, k_scr, heads, slots * heads)
            split_heads(raw.at[b % 2, 1], wide, v_scr, heads, slots * heads)
            for i in (0, 2):
                q_copy(b, i).wait_recv()
            for i in range(3):
                q_copy(b, i).wait_send()

        limit = pre_ref[jnp.minimum(b, rows - 1)] - me * slots

        def head(h, _):
            @pl.when(b < rows)
            def _():
                col = pl.ds(pl.multiple_of(h * 128, 128), 128)
                o, lse = attend_head(h, q_buf[b, :, col], k_scr, v_scr, kn[b, :, col], vn[b, :, col], s_scr, limit, bias[...], 256)
                q_buf[b, :, col] = o.astype(BF16)
                lse_scr[...] = jnp.where(head_lane == h, lse, lse_scr[...])

            @pl.when(h == 0)
            def _():
                @pl.when((b >= 1) & (b < rows + 1))
                def _():
                    precombine(b - 1)

                @pl.when((b >= 2) & (b < rows + 2))
                def _():
                    o_hop(b - 2, 2)

            @pl.when(h == 1)
            def _():
                @pl.when(b == 6)
                def _():
                    for i in (2, 4, 5, 6):
                        w_copy(i).wait_recv()

                @pl.when(b == rows + 2)
                def _():
                    project_out(groups - 1)

            @pl.when(h == 2)
            def _():
                @pl.when((b >= 2) & (b < rows + 2))
                def _():
                    o_hop(b - 2, 3)

                @pl.when((b >= 1) & (b < rows + 1))
                def _():
                    finish(b - 1)

            @pl.when(h == 3)
            def _():
                @pl.when(b == 1)
                def _():
                    w_copy(0).wait_recv()
                    w_copy(3).start()
                    w_copy(4).start()

                @pl.when(b == 4)
                def _():
                    w_copy(1).wait_recv()
                    w_copy(3).wait_recv()
                    w_copy(5).start()
                    w_copy(6).start()

                @pl.when((b >= 6) & (b < 6 + groups - 1))
                def _():
                    project_out(b - 6)
            return 0

        lax.fori_loop(0, heads, head, 0)

        @pl.when(b < rows)
        def _():
            l_buf[b] = jnp.transpose(lse_scr[...])[0:8, :]
            for i in range(4):
                p_copy(b, i).start()
        return 0

    lax.fori_loop(0, rows + 3, row, 0)

    for g in range(groups):
        out_copy(g).wait()
    for cpy in outs:
        cpy.wait()

    def sent_g(g, _):
        for i in range(1, n_tp):
            st_copy(g, i).wait_send()
        return 0

    lax.fori_loop(0, groups, sent_g, 0)

    def sent_b(b, _):
        for i in range(6):
            p_copy(b, i).wait_send()
        hop_sent(lambda o: o_all.at[o, b], lambda d, i: z_s.at[b, d * last + i], lambda d, i: z_r.at[b, d * last + i])
        return 0

    lax.fori_loop(0, rows, sent_b, 0)
    hop_sent(lambda o: wf.at[o, js, :], lambda d, i: w_s.at[d * last + i], lambda d, i: w_r.at[d * last + i])
    for i in range(7):
        w_copy(i).wait_send()


def solution(mesh):
    n_tp = mesh.shape['tp']

    def local_step(x_chunk, w_query, w_key, w_value, w_out, q_gain, k_gain, post_gain, cache_k, cache_v, prefix_len):
        rows, toks, model = x_chunk.shape
        slots, heads, dim = cache_k.shape[1:]
        width = heads * dim
        n_q = 4 * toks
        positions = prefix_len[:, None] + lax.axis_index('cp') * toks + jnp.arange(toks, dtype=jnp.int32)[None, :]
        inv_freq = ROPE_BASE ** (-(jnp.arange(dim // 2, dtype=F32) * 2.0 / dim))
        angles = positions.astype(F32)[..., None] * inv_freq
        cos, sin = jnp.cos(angles), jnp.sin(angles)
        cos = jnp.concatenate([cos, cos], axis=-1)
        sin = jnp.concatenate([-sin, sin], axis=-1)
        any_ = pl.BlockSpec(memory_space=pl.ANY)
        vm = pl.BlockSpec(memory_space=pltpu.VMEM)
        dma = pltpu.SemaphoreType.DMA
        last = n_tp - 1
        scratch = [
            pltpu.VMEM((rows, toks, model), BF16), pltpu.VMEM((3, model, width), BF16), pltpu.VMEM((n_tp, width, model), BF16),
            pltpu.VMEM((rows, n_q, width), BF16), pltpu.VMEM((rows, toks, width), BF16), pltpu.VMEM((rows, toks, width), BF16),
            pltpu.VMEM((rows, toks, width), BF16), pltpu.VMEM((rows, toks, width), BF16), pltpu.VMEM((rows, toks, width), BF16),
            pltpu.VMEM((rows, 8, toks), F32), pltpu.VMEM((rows, 8, toks), F32), pltpu.VMEM((rows, 8, toks), F32),
            pltpu.VMEM((rows, toks, width), BF16), pltpu.VMEM((rows, 8, toks), F32), pltpu.VMEM((rows, 8, n_q), F32),
            pltpu.VMEM((n_tp, rows, toks, width), BF16), pltpu.VMEM((rows // 2, n_tp, 8, 2 * toks), F32),
            pltpu.VMEM((2, 2, slots * heads, dim), BF16), pltpu.VMEM((1024, 128), F32),
            pltpu.VMEM((heads, slots, dim), BF16), pltpu.VMEM((heads, slots, dim), BF16),
            pltpu.VMEM((n_q, slots), F32), pltpu.VMEM((n_q, toks), F32), pltpu.VMEM((n_q, 128), F32),
            dma((5,)), dma((2, 2)), dma((rows // 2 + 2,)), dma((rows // 2, last)), dma((rows // 2, last)),
            dma((rows, 3)), dma((rows, 3)), dma((rows, 6)), dma((rows, 6)), dma((rows, 2 * last)), dma((rows, 2 * last)),
            dma((2 * last + 7,)), dma((2 * last + 7,)),
        ]
        flops = 2 * rows * toks * model * width * 3 + 4 * rows * n_q * slots * width + 2 * rows * toks * model * model
        out, ok, ov = pl.pallas_call(
            functools.partial(step_kernel, n_tp),
            in_specs=[pl.BlockSpec(memory_space=pltpu.SMEM)] + [any_] * 5 + [vm] * 5 + [any_] * 2,
            out_specs=[any_] * 3,
            out_shape=[jax.ShapeDtypeStruct((rows, toks, model), BF16), jax.ShapeDtypeStruct((rows, toks, width), BF16), jax.ShapeDtypeStruct((rows, toks, width), BF16)],
            scratch_shapes=scratch,
            compiler_params=pltpu.CompilerParams(collective_id=0, has_side_effects=True, vmem_limit_bytes=67043328),
            cost_estimate=pl.CostEstimate(flops=flops, bytes_accessed=4 * rows * slots * width, transcendentals=rows * n_q * slots * heads),
            name="step",
        )(prefix_len, x_chunk, w_query, w_key, w_value, w_out, q_gain.reshape(1, width), k_gain.reshape(1, width), post_gain.reshape(1, model),
          cos, sin, cache_k.reshape(rows, slots * heads, dim), cache_v.reshape(rows, slots * heads, dim))
        return out, ok.reshape(rows, toks, heads, dim), ov.reshape(rows, toks, heads, dim)

    x_spec = P('dp', 'cp', None)
    head_spec = P('dp', 'cp', 'tp', None)
    in_specs = (x_spec, P(None, 'tp'), P(None, 'tp'), P(None, 'tp'), P('tp', None), P('tp'), P('tp'), P(None), head_spec, head_spec, P('dp'))
    out_specs = (x_spec, head_spec, head_spec)
    return jax.shard_map(local_step, mesh=mesh, in_specs=in_specs, out_specs=out_specs, check_vma=False)
```

```python
import functools
import jax
import jax.numpy as jnp
from jax import lax
from jax.experimental import pallas as pl
from jax.experimental.pallas import tpu as pltpu
from jax.sharding import PartitionSpec as P

NORM_EPS = 1e-6
ROPE_BASE = 500000.0
MASK_VALUE = -1e30
LOG2E = 1.4426950408889634
MESH = pl.DeviceIdType.MESH
NT = (((1,), (1,)), ((), ()))
F32 = jnp.float32
BF16 = jnp.bfloat16


def split_heads(raw_ref, wide_ref, out_ref, heads, rows):
    step = wide_ref.shape[0]
    per = step // heads

    def body(i, _):
        wide_ref[...] = raw_ref[pl.ds(i * step, step), :].astype(F32)
        for h in range(heads):
            out_ref[h, pl.ds(i * per, per), 0:128] = wide_ref[pl.ds(h, per, stride=heads), :].astype(BF16)
        return 0

    lax.fori_loop(0, rows // step, body, 0)


SCALE = (128 ** -0.5) * LOG2E
TILE = 256


def scores(q, h, kc, bias, k_ref, s_ref, limit):
    n_t = k_ref.shape[1] // TILE
    lane = lax.broadcasted_iota(jnp.int32, (1, TILE), 1)
    s = lax.dot_general(q, kc, NT, preferred_element_type=F32)
    s = jnp.where(bias >= 0, s, MASK_VALUE)
    s_ref[:, n_t * TILE:n_t * TILE + 128] = s
    mx = s
    for j in range(n_t):
        s = lax.dot_general(q, k_ref[h, j * TILE:(j + 1) * TILE, :], NT, preferred_element_type=F32)
        s = jnp.where(lane + j * TILE < limit, s, MASK_VALUE)
        s_ref[:, j * TILE:(j + 1) * TILE] = s
        for u in range(TILE // 128):
            mx = jnp.maximum(mx, s[:, u * 128:(u + 1) * 128])
    return jnp.max(mx, axis=1, keepdims=True) * SCALE


def weigh(top, h, vc, v_ref, s_ref):
    n_t = v_ref.shape[1] // TILE
    acc = None
    for j in range(n_t):
        p = jnp.exp2(s_ref[:, j * TILE:(j + 1) * TILE] * SCALE - top)
        d = jnp.dot(p.astype(BF16), v_ref[h, j * TILE:(j + 1) * TILE, :], preferred_element_type=F32)
        acc = d if acc is None else acc + d
    p = jnp.exp2(s_ref[:, n_t * TILE:n_t * TILE + 128] * SCALE - top)
    return acc + jnp.dot(p.astype(BF16), vc, preferred_element_type=F32)


def attend_head(h, q_ref, kc, vc, k_ref, v_ref, s_ref, limit, bias_ref, lse_ref):
    col = pl.ds(pl.multiple_of(h * 128, 128), 128)
    half = q_ref.shape[0] // 2
    vc = jnp.concatenate([vc, jnp.ones(vc.shape, BF16)], axis=1)
    parts = [slice(r * half, (r + 1) * half) for r in range(2)]
    tops = [scores(q_ref[rs, col], h, kc, bias_ref[rs, :], k_ref, s_ref.at[rs], limit) for rs in parts]
    lane = lax.broadcasted_iota(jnp.int32, (half, 128), 1)
    for rs, top in zip(parts, tops):
        acc = weigh(top, h, vc, v_ref, s_ref.at[rs])
        den = acc[:, 128:]
        q_ref[rs, col] = (acc[:, :128] * (1.0 / den)).astype(BF16)
        lse_ref[rs, :] = jnp.where(lane == h, top + jnp.log2(den), lse_ref[rs, :])


def step_kernel(n_tp, pre_ref, x_hbm, wq_hbm, wk_hbm, wv_hbm, wo_hbm, gain_ref, cos_ref, sin_ref, ck_hbm, cv_hbm,
                out_hbm, ok_hbm, ov_hbm,
                x_v, wqkv, wf, q_buf, kn, vn, rA, rB, rC, lA, lB, lC, c_o, c_l, l_buf, o_all, st,
                raw, wide, k_scr, v_scr, s_scr, bias, lse_scr,
                in_sem, kv_sem, out_sem, st_s, st_r, q_s, q_r, p_s, p_r, z_s, z_r, w_s, w_r):
    rows, toks, model = x_v.shape
    heads, slots = k_scr.shape[0], k_scr.shape[1]
    width = heads * 128
    groups = rows // 2
    gt = 2 * toks
    dp, z, me = lax.axis_index('dp'), lax.axis_index('tp'), lax.axis_index('cp')
    partner = me + 1 - 2 * (me % 2)
    counter = (me + 2) % 4
    diag = 3 - me
    last = n_tp - 1
    piece = wo_hbm.shape[0] // 8

    def remote(src, dst, ss, rs, **dev):
        return pltpu.make_async_remote_copy(src_ref=src, dst_ref=dst, send_sem=ss, recv_sem=rs, device_id=dev, device_id_type=MESH)

    loads = [pltpu.make_async_copy(x_hbm, x_v, in_sem.at[0])]
    for i, w in enumerate((wq_hbm, wk_hbm, wv_hbm)):
        loads.append(pltpu.make_async_copy(w, wqkv.at[i], in_sem.at[1 + i]))
    js = pl.ds(pl.multiple_of((dp * 4 + me) * piece, piece), piece)
    w_local = pltpu.make_async_copy(wo_hbm.at[js, :], wf.at[z, js, :], in_sem.at[4])
    w_local.start()
    for cpy in loads:
        cpy.start()

    def kv_copies(b):
        par = b % 2
        return (pltpu.make_async_copy(ck_hbm.at[b], raw.at[par, 0], kv_sem.at[par, 0]),
                pltpu.make_async_copy(cv_hbm.at[b], raw.at[par, 1], kv_sem.at[par, 1]))

    for cpy in kv_copies(0):
        cpy.start()

    barrier = pltpu.get_barrier_semaphore()
    for i in range(1, n_tp):
        pl.semaphore_signal(barrier, inc=1, device_id={'tp': (z + i) % n_tp}, device_id_type=MESH)
    pl.semaphore_signal(barrier, inc=1, device_id={'cp': partner}, device_id_type=MESH)
    pl.semaphore_signal(barrier, inc=1, device_id={'cp': counter}, device_id_type=MESH)
    pl.semaphore_signal(barrier, inc=1, device_id={'dp': 1 - dp}, device_id_type=MESH)
    pl.semaphore_wait(barrier, n_tp + 2)

    def hop(buf, send, recv, k, wait_only=False, start=True):
        if k > 1:
            @pl.when(z - (k - 1) >= 0)
            def _():
                remote(buf(z - (k - 1)), buf(z - (k - 1)), send(0, k - 2), recv(0, k - 2), tp=z).wait_recv()

            @pl.when(z + (k - 1) <= last)
            def _():
                remote(buf(z + (k - 1)), buf(z + (k - 1)), send(1, k - 2), recv(1, k - 2), tp=z).wait_recv()
        if k <= last:
            @pl.when((z - (k - 1) >= 0) & (z < last))
            def _():
                remote(buf(z - (k - 1)), buf(z - (k - 1)), send(0, k - 1), recv(0, k - 1), tp=z + 1).start()

            @pl.when((z + (k - 1) <= last) & (z > 0))
            def _():
                remote(buf(z + (k - 1)), buf(z + (k - 1)), send(1, k - 1), recv(1, k - 1), tp=z - 1).start()

    def hop_sent(buf, send, recv):
        for k in range(1, last + 1):
            @pl.when((z - (k - 1) >= 0) & (z < last))
            def _():
                remote(buf(z - (k - 1)), buf(z - (k - 1)), send(0, k - 1), recv(0, k - 1), tp=z).wait_send()

            @pl.when((z + (k - 1) <= last) & (z > 0))
            def _():
                remote(buf(z + (k - 1)), buf(z + (k - 1)), send(1, k - 1), recv(1, k - 1), tp=z).wait_send()

    def w_hop(k):
        hop(lambda o: wf.at[o, js, :], lambda d, i: w_s.at[d * last + i], lambda d, i: w_r.at[d * last + i], k)

    def o_hop(b, k):
        hop(lambda o: o_all.at[o, b], lambda d, i: z_s.at[b, d * last + i], lambda d, i: z_r.at[b, d * last + i], k)

    w_local.wait()
    w_hop(1)

    qi = lax.broadcasted_iota(jnp.int32, (toks, toks), 0)
    ki = lax.broadcasted_iota(jnp.int32, (toks, toks), 1)
    for s, blk in enumerate((me, partner, counter, diag)):
        bias[s * toks:(s + 1) * toks, :] = jnp.where(ki - qi <= (blk - me) * toks, 0.0, -1.0)
    lse_scr[...] = jnp.zeros(lse_scr.shape, F32)
    v_scr[:, :, 128:] = jnp.ones((heads, slots, 128), BF16)

    for cpy in loads:
        cpy.wait()

    def st_copy(g, i):
        return remote(st.at[g, 0], st.at[g, i], st_s.at[g, i - 1], st_r.at[g, i - 1], tp=(z + i) % n_tp)

    def q_copy(b, i):
        src = q_buf.at[b, pl.ds(0 if i < 2 else 2 * toks, toks), :]
        dst = q_buf.at[b, pl.ds((i + 1) * toks, toks), :]
        return remote(src, dst, q_s.at[b, i], q_r.at[b, i], cp=counter if i == 1 else partner)

    def project(g):
        xg = x_v[pl.ds(2 * g, 2)].reshape(gt, model)
        cols = pl.ds(pl.multiple_of(g * width, width), width)
        q = jnp.dot(xg, wqkv[0], preferred_element_type=F32)
        s_scr[0:gt, cols] = q
        k = jnp.dot(xg, wqkv[1], preferred_element_type=F32)
        s_scr[gt:2 * gt, cols] = k
        lane = lax.broadcasted_iota(jnp.int32, (gt, 128), 1)
        sq = jnp.sum(q * q, axis=1, keepdims=True)
        sk = jnp.sum(k * k, axis=1, keepdims=True)
        sums = jnp.where(lane == 0, sq, jnp.where(lane == 1, sk, 0.0))
        st[g, 0] = jnp.transpose(sums)[0:8, :]
        v = jnp.dot(xg, wqkv[2], preferred_element_type=F32)
        for i in range(1, n_tp):
            st_copy(g, i).start()
        vn[pl.ds(2 * g, 2)] = v.astype(BF16).reshape(2, toks, width)

    def normalize(g):
        for i in range(1, n_tp):
            st_copy(g, i).wait_recv()
        tot = st[g, 0]
        for i in range(1, n_tp):
            tot = tot + st[g, i]
        inv = jnp.transpose(lax.rsqrt(tot / (width * n_tp) + NORM_EPS))
        for t, (gain, base) in enumerate(((0, 0), (width, gt))):
            for h in range(heads):
                u = s_scr[base:base + gt, pl.ds(pl.multiple_of(g * width + h * 128, 128), 128)]
                u = u * inv[:, t:t + 1] * gain_ref[0:1, gain + h * 128:gain + (h + 1) * 128]
                cos = cos_ref[pl.ds(2 * g, 2)].reshape(gt, 128)
                sin = sin_ref[pl.ds(2 * g, 2)].reshape(gt, 128)
                u = (u * cos + pltpu.roll(u, 64, 1) * sin).astype(BF16).reshape(2, toks, 128)
                if t == 0:
                    q_buf[pl.ds(2 * g, 2), 0:toks, h * 128:(h + 1) * 128] = u
                else:
                    kn[pl.ds(2 * g, 2), :, h * 128:(h + 1) * 128] = u
        for r in range(2):
            q_copy(2 * g + r, 0).start()
            q_copy(2 * g + r, 1).start()

    def front(g, _):
        @pl.when(g < groups)
        def _():
            project(g)

        @pl.when(g == 1)
        def _():
            w_hop(2)

        @pl.when(g == 2)
        def _():
            w_hop(3)

        @pl.when(g > 0)
        def _():
            normalize(g - 1)
        return 0

    lax.fori_loop(0, groups + 1, front, 0)

    outs = (pltpu.make_async_copy(kn, ok_hbm, out_sem.at[groups]), pltpu.make_async_copy(vn, ov_hbm, out_sem.at[groups + 1]))
    for cpy in outs:
        cpy.start()

    nw = 2 * last

    def wslice(d, c):
        return wf.at[:, pl.ds(pl.multiple_of((d * 4 + c) * piece, piece), piece), :]

    def w_copy(i):
        ref = (wslice(dp, me), wslice(dp, me), wslice(dp, me), wslice(dp, counter), wslice(dp, counter), wslice(1 - dp, me), wslice(1 - dp, counter))[i]
        dev = ({'cp': counter}, {'dp': 1 - dp}, {'cp': partner}, {'dp': 1 - dp}, {'cp': partner}, {'cp': partner}, {'cp': partner})[i]
        return remote(ref, ref, w_s.at[nw + i], w_r.at[nw + i], **dev)

    w_hop(4)
    for i in range(3):
        w_copy(i).start()

    def forward_q(b):
        q_copy(b, 1).wait_recv()
        q_copy(b, 2).start()

    forward_q(0)

    def p_copy(b, i):
        if i < 4:
            s = 1 if i < 2 else 3
            src = (q_buf.at[b, pl.ds(s * toks, toks), :], l_buf.at[b, :, pl.ds(s * toks, toks)])[i % 2]
        else:
            src = (c_o.at[b], c_l.at[b])[i % 2]
        dst = (rA.at[b], lA.at[b], rB.at[b], lB.at[b], rC.at[b], lC.at[b])[i]
        return remote(src, dst, p_s.at[b, i], p_r.at[b, i], cp=partner if i < 4 else counter)

    def blend(parts, dst):
        top = functools.reduce(jnp.maximum, [e for _, e in parts])
        ws = [jnp.exp2(e - top) for _, e in parts]
        den = functools.reduce(jnp.add, ws)
        cols = [jnp.transpose(w / den) for w in ws]
        for h in range(heads):
            hs = slice(h * 128, (h + 1) * 128)
            acc = functools.reduce(jnp.add, [c[:, h:h + 1] * v[:, hs].astype(F32) for c, (v, _) in zip(cols, parts)])
            dst[:, hs] = acc.astype(BF16)
        return top + jnp.log2(den)

    def precombine(b):
        p_copy(b, 2).wait_recv()
        p_copy(b, 3).wait_recv()
        c_l[b] = blend([(q_buf.at[b, pl.ds(2 * toks, toks), :], l_buf[b, :, 2 * toks:3 * toks]), (rB.at[b], lB[b])], c_o.at[b])
        p_copy(b, 4).start()
        p_copy(b, 5).start()

    def finish(b):
        for i in (0, 1, 4, 5):
            p_copy(b, i).wait_recv()
        blend([(q_buf.at[b, pl.ds(0, toks), :], l_buf[b, :, 0:toks]), (rA.at[b], lA[b]), (rC.at[b], lC[b])], o_all.at[z, b])
        o_hop(b, 1)

    def out_copy(g):
        return pltpu.make_async_copy(x_v.at[pl.ds(2 * g, 2)], out_hbm.at[pl.ds(2 * g, 2)], out_sem.at[g])

    def project_out(g):
        o_hop(2 * g, 4)
        o_hop(2 * g + 1, 4)

        def chunk(n, ss):
            cols = pl.ds(pl.multiple_of(n * 512, 512), 512)
            y = None
            for t in range(n_tp):
                d = jnp.dot(o_all[t, pl.ds(2 * g, 2)].reshape(gt, width), wf[t, :, cols], preferred_element_type=F32)
                y = d if y is None else y + d
            s_scr[0:gt, cols] = y
            return ss + jnp.sum(y * y, axis=1, keepdims=True)

        ss = lax.fori_loop(0, model // 512, chunk, jnp.zeros((gt, 1), F32))
        inv = lax.rsqrt(ss / model + NORM_EPS)
        for n in range(model // 512):
            cols = slice(n * 512, (n + 1) * 512)
            y = s_scr[0:gt, cols] * inv * gain_ref[0:1, 2 * width + n * 512:2 * width + (n + 1) * 512]
            y = x_v[pl.ds(2 * g, 2), :, cols].reshape(gt, 512).astype(F32) + y
            x_v[pl.ds(2 * g, 2), :, cols] = y.astype(BF16).reshape(2, toks, 512)
        out_copy(g).start()

    def row(b, _):
        @pl.when(b < rows)
        def _():
            for cpy in kv_copies(b):
                cpy.wait()

            @pl.when(b + 1 < rows)
            def _():
                for cpy in kv_copies(b + 1):
                    cpy.start()
                forward_q(b + 1)

            split_heads(raw.at[b % 2, 0], wide, k_scr, heads, slots * heads)
            split_heads(raw.at[b % 2, 1], wide, v_scr, heads, slots * heads)
            for i in (0, 2):
                q_copy(b, i).wait_recv()
            for i in range(3):
                q_copy(b, i).wait_send()

        limit = pre_ref[jnp.minimum(b, rows - 1)] - me * slots

        def head(h, _):
            @pl.when(b < rows)
            def _():
                col = pl.ds(pl.multiple_of(h * 128, 128), 128)
                attend_head(h, q_buf.at[b], kn[b, :, col], vn[b, :, col], k_scr, v_scr, s_scr, limit, bias, lse_scr)

            @pl.when(h == 0)
            def _():
                @pl.when((b >= 1) & (b < rows + 1))
                def _():
                    precombine(b - 1)

                @pl.when((b >= 2) & (b < rows + 2))
                def _():
                    o_hop(b - 2, 2)

            @pl.when(h == 1)
            def _():
                @pl.when(b == 6)
                def _():
                    for i in (2, 4, 5, 6):
                        w_copy(i).wait_recv()

                @pl.when(b == rows + 2)
                def _():
                    project_out(groups - 1)

            @pl.when(h == 2)
            def _():
                @pl.when((b >= 2) & (b < rows + 2))
                def _():
                    o_hop(b - 2, 3)

                @pl.when((b >= 1) & (b < rows + 1))
                def _():
                    finish(b - 1)

            @pl.when(h == 3)
            def _():
                @pl.when(b == 1)
                def _():
                    w_copy(0).wait_recv()
                    w_copy(3).start()
                    w_copy(4).start()

                @pl.when(b == 4)
                def _():
                    w_copy(1).wait_recv()
                    w_copy(3).wait_recv()
                    w_copy(5).start()
                    w_copy(6).start()

                @pl.when((b >= 6) & (b < 6 + groups - 1))
                def _():
                    project_out(b - 6)
            return 0

        lax.fori_loop(0, heads, head, 0)

        @pl.when(b < rows)
        def _():
            l_buf[b] = jnp.transpose(lse_scr[...])[0:8, :]
            for i in range(4):
                p_copy(b, i).start()
        return 0

    lax.fori_loop(0, rows + 3, row, 0)

    for g in range(groups):
        out_copy(g).wait()
    for cpy in outs:
        cpy.wait()

    def sent_g(g, _):
        for i in range(1, n_tp):
            st_copy(g, i).wait_send()
        return 0

    lax.fori_loop(0, groups, sent_g, 0)

    def sent_b(b, _):
        for i in range(6):
            p_copy(b, i).wait_send()
        hop_sent(lambda o: o_all.at[o, b], lambda d, i: z_s.at[b, d * last + i], lambda d, i: z_r.at[b, d * last + i])
        return 0

    lax.fori_loop(0, rows, sent_b, 0)
    hop_sent(lambda o: wf.at[o, js, :], lambda d, i: w_s.at[d * last + i], lambda d, i: w_r.at[d * last + i])
    for i in range(7):
        w_copy(i).wait_send()


def solution(mesh):
    n_tp = mesh.shape['tp']

    def local_step(x_chunk, w_query, w_key, w_value, w_out, q_gain, k_gain, post_gain, cache_k, cache_v, prefix_len):
        rows, toks, model = x_chunk.shape
        slots, heads, dim = cache_k.shape[1:]
        width = heads * dim
        n_q = 4 * toks
        positions = prefix_len[:, None] + lax.axis_index('cp') * toks + jnp.arange(toks, dtype=jnp.int32)[None, :]
        inv_freq = ROPE_BASE ** (-(jnp.arange(dim // 2, dtype=F32) * 2.0 / dim))
        angles = positions.astype(F32)[..., None] * inv_freq
        cos, sin = jnp.cos(angles), jnp.sin(angles)
        cos = jnp.concatenate([cos, cos], axis=-1)
        sin = jnp.concatenate([-sin, sin], axis=-1)
        any_ = pl.BlockSpec(memory_space=pl.ANY)
        vm = pl.BlockSpec(memory_space=pltpu.VMEM)
        dma = pltpu.SemaphoreType.DMA
        last = n_tp - 1
        scratch = [
            pltpu.VMEM((rows, toks, model), BF16), pltpu.VMEM((3, model, width), BF16), pltpu.VMEM((n_tp, width, model), BF16),
            pltpu.VMEM((rows, n_q, width), BF16), pltpu.VMEM((rows, toks, width), BF16), pltpu.VMEM((rows, toks, width), BF16),
            pltpu.VMEM((rows, toks, width), BF16), pltpu.VMEM((rows, toks, width), BF16), pltpu.VMEM((rows, toks, width), BF16),
            pltpu.VMEM((rows, 8, toks), F32), pltpu.VMEM((rows, 8, toks), F32), pltpu.VMEM((rows, 8, toks), F32),
            pltpu.VMEM((rows, toks, width), BF16), pltpu.VMEM((rows, 8, toks), F32), pltpu.VMEM((rows, 8, n_q), F32),
            pltpu.VMEM((n_tp, rows, toks, width), BF16), pltpu.VMEM((rows // 2, n_tp, 8, 2 * toks), F32),
            pltpu.VMEM((2, 2, slots * heads, dim), BF16), pltpu.VMEM((1024, 128), F32),
            pltpu.VMEM((heads, slots, dim), BF16), pltpu.VMEM((heads, slots, 2 * dim), BF16),
            pltpu.VMEM((n_q, slots + toks), F32), pltpu.VMEM((n_q, toks), F32), pltpu.VMEM((n_q, 128), F32),
            dma((5,)), dma((2, 2)), dma((rows // 2 + 2,)), dma((rows // 2, last)), dma((rows // 2, last)),
            dma((rows, 3)), dma((rows, 3)), dma((rows, 6)), dma((rows, 6)), dma((rows, 2 * last)), dma((rows, 2 * last)),
            dma((2 * last + 7,)), dma((2 * last + 7,)),
        ]
        flops = 2 * rows * toks * model * width * 3 + 4 * rows * n_q * slots * width + 2 * rows * toks * model * model
        out, ok, ov = pl.pallas_call(
            functools.partial(step_kernel, n_tp),
            in_specs=[pl.BlockSpec(memory_space=pltpu.SMEM)] + [any_] * 5 + [vm] * 3 + [any_] * 2,
            out_specs=[any_] * 3,
            out_shape=[jax.ShapeDtypeStruct((rows, toks, model), BF16), jax.ShapeDtypeStruct((rows, toks, width), BF16), jax.ShapeDtypeStruct((rows, toks, width), BF16)],
            scratch_shapes=scratch,
            compiler_params=pltpu.CompilerParams(collective_id=0, has_side_effects=True, vmem_limit_bytes=67043328),
            cost_estimate=pl.CostEstimate(flops=flops, bytes_accessed=4 * rows * slots * width, transcendentals=rows * n_q * slots * heads),
            name="step",
        )(prefix_len, x_chunk, w_query, w_key, w_value, w_out, jnp.concatenate([q_gain, k_gain, post_gain]).astype(F32).reshape(1, 2 * width + model),
          cos, sin, cache_k.reshape(rows, slots * heads, dim), cache_v.reshape(rows, slots * heads, dim))
        return out, ok.reshape(rows, toks, heads, dim), ov.reshape(rows, toks, heads, dim)

    x_spec = P('dp', 'cp', None)
    head_spec = P('dp', 'cp', 'tp', None)
    in_specs = (x_spec, P(None, 'tp'), P(None, 'tp'), P(None, 'tp'), P('tp', None), P('tp'), P('tp'), P(None), head_spec, head_spec, P('dp'))
    out_specs = (x_spec, head_spec, head_spec)
    return jax.shard_map(local_step, mesh=mesh, in_specs=in_specs, out_specs=out_specs, check_vma=False)
```

```python
import functools
import jax
import jax.numpy as jnp
from jax import lax
from jax.experimental import pallas as pl
from jax.experimental.pallas import tpu as pltpu
from jax.sharding import PartitionSpec as P

NORM_EPS = 1e-6
ROPE_BASE = 500000.0
MASK_VALUE = -1e30
LOG2E = 1.4426950408889634
MESH = pl.DeviceIdType.MESH
NT = (((1,), (1,)), ((), ()))
F32 = jnp.float32
BF16 = jnp.bfloat16


def split_heads(raw_ref, wide_ref, out_ref, heads, rows):
    step = wide_ref.shape[0]
    per = step // heads

    def body(i, _):
        wide_ref[...] = raw_ref[pl.ds(i * step, step), :].astype(F32)
        for h in range(heads):
            out_ref[h, pl.ds(i * per, per), 0:128] = wide_ref[pl.ds(h, per, stride=heads), :].astype(BF16)
        return 0

    lax.fori_loop(0, rows // step, body, 0)


SCALE = (128 ** -0.5) * LOG2E
TILE = 256


def scores(q, h, kc, bias, k_ref, s_ref, limit):
    n_t = k_ref.shape[1] // TILE
    lane = lax.broadcasted_iota(jnp.int32, (1, TILE), 1)
    s = lax.dot_general(q, kc, NT, preferred_element_type=F32)
    s = jnp.where(bias >= 0, s, MASK_VALUE)
    s_ref[:, n_t * TILE:n_t * TILE + 128] = s
    mx = s
    for j in range(n_t):
        s = lax.dot_general(q, k_ref[h, j * TILE:(j + 1) * TILE, :], NT, preferred_element_type=F32)
        s = jnp.where(lane + j * TILE < limit, s, MASK_VALUE)
        s_ref[:, j * TILE:(j + 1) * TILE] = s
        for u in range(TILE // 128):
            mx = jnp.maximum(mx, s[:, u * 128:(u + 1) * 128])
    return jnp.max(mx, axis=1, keepdims=True) * SCALE


def weigh(top, h, vc, v_ref, s_ref):
    n_t = v_ref.shape[1] // TILE
    acc = None
    for j in range(n_t):
        p = jnp.exp2(s_ref[:, j * TILE:(j + 1) * TILE] * SCALE - top)
        d = jnp.dot(p.astype(BF16), v_ref[h, j * TILE:(j + 1) * TILE, :], preferred_element_type=F32)
        acc = d if acc is None else acc + d
    p = jnp.exp2(s_ref[:, n_t * TILE:n_t * TILE + 128] * SCALE - top)
    return acc + jnp.dot(p.astype(BF16), vc, preferred_element_type=F32)


def attend_head(h, q_ref, kc, vc, k_ref, v_ref, s_ref, limit, bias_ref, lse_ref):
    col = pl.ds(pl.multiple_of(h * 128, 128), 128)
    half = q_ref.shape[0] // 2
    vc = jnp.concatenate([vc, jnp.ones(vc.shape, BF16)], axis=1)
    parts = [slice(r * half, (r + 1) * half) for r in range(2)]
    tops = [scores(q_ref[rs, col], h, kc, bias_ref[rs, :], k_ref, s_ref.at[rs], limit) for rs in parts]
    lane = lax.broadcasted_iota(jnp.int32, (half, 128), 1)
    for rs, top in zip(parts, tops):
        acc = weigh(top, h, vc, v_ref, s_ref.at[rs])
        den = acc[:, 128:]
        q_ref[rs, col] = (acc[:, :128] * (1.0 / den)).astype(BF16)
        lse_ref[rs, :] = jnp.where(lane == h, top + jnp.log2(den), lse_ref[rs, :])


def step_kernel(n_tp, pre_ref, x_hbm, wq_hbm, wk_hbm, wv_hbm, wo_hbm, gain_ref, cos_ref, sin_ref, ck_hbm, cv_hbm,
                out_hbm, ok_hbm, ov_hbm,
                x_v, wqkv, wf, q_buf, kn, vn, rA, rB, rC, lA, lB, lC, c_o, c_l, l_buf, o_all, st,
                raw, wide, k_scr, v_scr, s_scr, bias, lse_scr,
                in_sem, kv_sem, out_sem, st_s, st_r, q_s, q_r, p_s, p_r, z_s, z_r, w_s, w_r):
    rows, toks, model = x_v.shape
    heads, slots = k_scr.shape[0], k_scr.shape[1]
    width = heads * 128
    groups = rows // 2
    gt = 2 * toks
    dp, z, me = lax.axis_index('dp'), lax.axis_index('tp'), lax.axis_index('cp')
    partner = me + 1 - 2 * (me % 2)
    counter = (me + 2) % 4
    diag = 3 - me
    last = n_tp - 1
    piece = wo_hbm.shape[0] // 8

    def remote(src, dst, ss, rs, **dev):
        return pltpu.make_async_remote_copy(src_ref=src, dst_ref=dst, send_sem=ss, recv_sem=rs, device_id=dev, device_id_type=MESH)

    def x_copy(g):
        return pltpu.make_async_copy(x_hbm.at[pl.ds(2 * g, 2)], x_v.at[pl.ds(2 * g, 2)], in_sem.at[4 + g])

    w_copies = [pltpu.make_async_copy(w, wqkv.at[i], in_sem.at[1 + i]) for i, w in enumerate((wq_hbm, wk_hbm, wv_hbm))]
    js = pl.ds(pl.multiple_of((dp * 4 + me) * piece, piece), piece)
    w_local = pltpu.make_async_copy(wo_hbm.at[js, :], wf.at[z, js, :], in_sem.at[0])
    w_copies[0].start()
    x_copy(0).start()
    w_local.start()
    w_copies[1].start()
    w_copies[2].start()
    for g in range(1, groups):
        x_copy(g).start()

    def kv_copies(b):
        par = b % 2
        return (pltpu.make_async_copy(ck_hbm.at[b], raw.at[par, 0], kv_sem.at[par, 0]),
                pltpu.make_async_copy(cv_hbm.at[b], raw.at[par, 1], kv_sem.at[par, 1]))

    for cpy in kv_copies(0):
        cpy.start()

    barrier = pltpu.get_barrier_semaphore()
    for i in range(1, n_tp):
        pl.semaphore_signal(barrier, inc=1, device_id={'tp': (z + i) % n_tp}, device_id_type=MESH)
    pl.semaphore_signal(barrier, inc=1, device_id={'cp': partner}, device_id_type=MESH)
    pl.semaphore_signal(barrier, inc=1, device_id={'cp': counter}, device_id_type=MESH)
    pl.semaphore_signal(barrier, inc=1, device_id={'dp': 1 - dp}, device_id_type=MESH)
    pl.semaphore_wait(barrier, n_tp + 2)

    def hop(buf, send, recv, k, wait_only=False, start=True):
        if k > 1:
            @pl.when(z - (k - 1) >= 0)
            def _():
                remote(buf(z - (k - 1)), buf(z - (k - 1)), send(0, k - 2), recv(0, k - 2), tp=z).wait_recv()

            @pl.when(z + (k - 1) <= last)
            def _():
                remote(buf(z + (k - 1)), buf(z + (k - 1)), send(1, k - 2), recv(1, k - 2), tp=z).wait_recv()
        if k <= last:
            @pl.when((z - (k - 1) >= 0) & (z < last))
            def _():
                remote(buf(z - (k - 1)), buf(z - (k - 1)), send(0, k - 1), recv(0, k - 1), tp=z + 1).start()

            @pl.when((z + (k - 1) <= last) & (z > 0))
            def _():
                remote(buf(z + (k - 1)), buf(z + (k - 1)), send(1, k - 1), recv(1, k - 1), tp=z - 1).start()

    def hop_sent(buf, send, recv):
        for k in range(1, last + 1):
            @pl.when((z - (k - 1) >= 0) & (z < last))
            def _():
                remote(buf(z - (k - 1)), buf(z - (k - 1)), send(0, k - 1), recv(0, k - 1), tp=z).wait_send()

            @pl.when((z + (k - 1) <= last) & (z > 0))
            def _():
                remote(buf(z + (k - 1)), buf(z + (k - 1)), send(1, k - 1), recv(1, k - 1), tp=z).wait_send()

    def w_hop(k):
        hop(lambda o: wf.at[o, js, :], lambda d, i: w_s.at[d * last + i], lambda d, i: w_r.at[d * last + i], k)

    def o_hop(b, k):
        hop(lambda o: o_all.at[o, b], lambda d, i: z_s.at[b, d * last + i], lambda d, i: z_r.at[b, d * last + i], k)

    w_local.wait()
    w_hop(1)

    qi = lax.broadcasted_iota(jnp.int32, (toks, toks), 0)
    ki = lax.broadcasted_iota(jnp.int32, (toks, toks), 1)
    for s, blk in enumerate((me, partner, counter, diag)):
        bias[s * toks:(s + 1) * toks, :] = jnp.where(ki - qi <= (blk - me) * toks, 0.0, -1.0)
    lse_scr[...] = jnp.zeros(lse_scr.shape, F32)
    v_scr[:, :, 128:] = jnp.ones((heads, slots, 128), BF16)

    def st_copy(g, i):
        return remote(st.at[g, 0], st.at[g, i], st_s.at[g, i - 1], st_r.at[g, i - 1], tp=(z + i) % n_tp)

    def q_copy(b, i):
        src = q_buf.at[b, pl.ds(0 if i < 2 else 2 * toks, toks), :]
        dst = q_buf.at[b, pl.ds((i + 1) * toks, toks), :]
        return remote(src, dst, q_s.at[b, i], q_r.at[b, i], cp=counter if i == 1 else partner)

    def project(g):
        x_copy(g).wait()

        @pl.when(g == 0)
        def _():
            w_copies[0].wait()
        xg = x_v[pl.ds(2 * g, 2)].reshape(gt, model)
        cols = pl.ds(pl.multiple_of(g * width, width), width)
        q = jnp.dot(xg, wqkv[0], preferred_element_type=F32)
        s_scr[0:gt, cols] = q

        @pl.when(g == 0)
        def _():
            w_copies[1].wait()
            w_copies[2].wait()
        k = jnp.dot(xg, wqkv[1], preferred_element_type=F32)
        s_scr[gt:2 * gt, cols] = k
        lane = lax.broadcasted_iota(jnp.int32, (gt, 128), 1)
        sq = jnp.sum(q * q, axis=1, keepdims=True)
        sk = jnp.sum(k * k, axis=1, keepdims=True)
        sums = jnp.where(lane == 0, sq, jnp.where(lane == 1, sk, 0.0))
        st[g, 0] = jnp.transpose(sums)[0:8, :]
        v = jnp.dot(xg, wqkv[2], preferred_element_type=F32)
        for i in range(1, n_tp):
            st_copy(g, i).start()
        vn[pl.ds(2 * g, 2)] = v.astype(BF16).reshape(2, toks, width)

    def normalize(g):
        for i in range(1, n_tp):
            st_copy(g, i).wait_recv()
        tot = st[g, 0]
        for i in range(1, n_tp):
            tot = tot + st[g, i]
        inv = jnp.transpose(lax.rsqrt(tot / (width * n_tp) + NORM_EPS))
        for t, (gain, base) in enumerate(((0, 0), (width, gt))):
            for h in range(heads):
                u = s_scr[base:base + gt, pl.ds(pl.multiple_of(g * width + h * 128, 128), 128)]
                u = u * inv[:, t:t + 1] * gain_ref[0:1, gain + h * 128:gain + (h + 1) * 128]
                cos = cos_ref[pl.ds(2 * g, 2)].reshape(gt, 128)
                sin = sin_ref[pl.ds(2 * g, 2)].reshape(gt, 128)
                u = (u * cos + pltpu.roll(u, 64, 1) * sin).astype(BF16).reshape(2, toks, 128)
                if t == 0:
                    q_buf[pl.ds(2 * g, 2), 0:toks, h * 128:(h + 1) * 128] = u
                else:
                    kn[pl.ds(2 * g, 2), :, h * 128:(h + 1) * 128] = u
        for r in range(2):
            q_copy(2 * g + r, 0).start()
            q_copy(2 * g + r, 1).start()

    def front(g, _):
        @pl.when(g < groups)
        def _():
            project(g)

        @pl.when(g > 0)
        def _():
            normalize(g - 1)
        return 0

    lax.fori_loop(0, groups + 1, front, 0)

    outs = (pltpu.make_async_copy(kn, ok_hbm, out_sem.at[groups]), pltpu.make_async_copy(vn, ov_hbm, out_sem.at[groups + 1]))
    for cpy in outs:
        cpy.start()

    nw = 2 * last

    def wslice(d, c):
        return pl.ds(pl.multiple_of((d * 4 + c) * piece, piece), piece)

    def w_send(k, t, ref, **dev):
        return remote(ref, ref, w_s.at[nw + k + t], w_r.at[nw + k + t], **dev)

    def w_y(t):
        return w_send(0, t, wf.at[t, wslice(dp, me), :], cp=counter)

    def w_x_own():
        return w_send(n_tp, 0, wf.at[:, wslice(dp, me), :], dp=1 - dp)

    def w_d_own():
        return w_send(n_tp, 1, wf.at[:, wslice(dp, me), :], cp=partner)

    def w_x_fwd(t):
        return w_send(n_tp + 2, t, wf.at[t, wslice(dp, counter), :], dp=1 - dp)

    def w_d_fwd(t):
        return w_send(2 * n_tp + 2, t, wf.at[t, wslice(dp, counter), :], cp=partner)

    def w_d_far(i):
        return w_send(3 * n_tp + 2, i, wf.at[:, wslice(1 - dp, (me, counter)[i]), :], cp=partner)

    w_hop(2)

    def forward_q(b):
        q_copy(b, 1).wait_recv()
        q_copy(b, 2).start()

    forward_q(0)

    def p_copy(b, i):
        if i < 4:
            s = 1 if i < 2 else 3
            src = (q_buf.at[b, pl.ds(s * toks, toks), :], l_buf.at[b, :, pl.ds(s * toks, toks)])[i % 2]
        else:
            src = (c_o.at[b], c_l.at[b])[i % 2]
        dst = (rA.at[b], lA.at[b], rB.at[b], lB.at[b], rC.at[b], lC.at[b])[i]
        return remote(src, dst, p_s.at[b, i], p_r.at[b, i], cp=partner if i < 4 else counter)

    def blend(parts, dst):
        top = functools.reduce(jnp.maximum, [e for _, e in parts])
        ws = [jnp.exp2(e - top) for _, e in parts]
        den = functools.reduce(jnp.add, ws)
        cols = [jnp.transpose(w / den) for w in ws]
        for h in range(heads):
            hs = slice(h * 128, (h + 1) * 128)
            acc = functools.reduce(jnp.add, [c[:, h:h + 1] * v[:, hs].astype(F32) for c, (v, _) in zip(cols, parts)])
            dst[:, hs] = acc.astype(BF16)
        return top + jnp.log2(den)

    def precombine(b):
        p_copy(b, 2).wait_recv()
        p_copy(b, 3).wait_recv()
        c_l[b] = blend([(q_buf.at[b, pl.ds(2 * toks, toks), :], l_buf[b, :, 2 * toks:3 * toks]), (rB.at[b], lB[b])], c_o.at[b])
        p_copy(b, 4).start()
        p_copy(b, 5).start()

    def finish(b):
        for i in (0, 1, 4, 5):
            p_copy(b, i).wait_recv()
        blend([(q_buf.at[b, pl.ds(0, toks), :], l_buf[b, :, 0:toks]), (rA.at[b], lA[b]), (rC.at[b], lC[b])], o_all.at[z, b])
        o_hop(b, 1)

    def out_copy(g):
        return pltpu.make_async_copy(x_v.at[pl.ds(2 * g, 2)], out_hbm.at[pl.ds(2 * g, 2)], out_sem.at[g])

    def project_out(g):
        o_hop(2 * g, 4)
        o_hop(2 * g + 1, 4)

        def chunk(n, ss):
            cols = pl.ds(pl.multiple_of(n * 512, 512), 512)
            y = None
            for t in range(n_tp):
                d = jnp.dot(o_all[t, pl.ds(2 * g, 2)].reshape(gt, width), wf[t, :, cols], preferred_element_type=F32)
                y = d if y is None else y + d
            s_scr[0:gt, cols] = y
            return ss + jnp.sum(y * y, axis=1, keepdims=True)

        ss = lax.fori_loop(0, model // 512, chunk, jnp.zeros((gt, 1), F32))
        inv = lax.rsqrt(ss / model + NORM_EPS)
        for n in range(model // 512):
            cols = slice(n * 512, (n + 1) * 512)
            y = s_scr[0:gt, cols] * inv * gain_ref[0:1, 2 * width + n * 512:2 * width + (n + 1) * 512]
            y = x_v[pl.ds(2 * g, 2), :, cols].reshape(gt, 512).astype(F32) + y
            x_v[pl.ds(2 * g, 2), :, cols] = y.astype(BF16).reshape(2, toks, 512)
        out_copy(g).start()

    def row(b, _):
        @pl.when(b < rows)
        def _():
            for cpy in kv_copies(b):
                cpy.wait()

            @pl.when(b + 1 < rows)
            def _():
                for cpy in kv_copies(b + 1):
                    cpy.start()
                forward_q(b + 1)

            split_heads(raw.at[b % 2, 0], wide, k_scr, heads, slots * heads)
            split_heads(raw.at[b % 2, 1], wide, v_scr, heads, slots * heads)
            for i in (0, 2):
                q_copy(b, i).wait_recv()
            for i in range(3):
                q_copy(b, i).wait_send()

        limit = pre_ref[jnp.minimum(b, rows - 1)] - me * slots

        def head(h, _):
            @pl.when(b < rows)
            def _():
                col = pl.ds(pl.multiple_of(h * 128, 128), 128)
                attend_head(h, q_buf.at[b], kn[b, :, col], vn[b, :, col], k_scr, v_scr, s_scr, limit, bias, lse_scr)

            @pl.when(h == 0)
            def _():
                @pl.when((b >= 1) & (b < rows + 1))
                def _():
                    precombine(b - 1)

                @pl.when((b >= 1) & (b < 1 + n_tp))
                def _():
                    w_y(b - 1).start()

                @pl.when((b >= 2) & (b < 2 + n_tp))
                def _():
                    w_y(b - 2).wait_recv()
                    w_x_fwd(b - 2).start()
                    w_d_fwd(b - 2).start()

                @pl.when((b >= 2) & (b < rows + 2))
                def _():
                    o_hop(b - 2, 2)

            @pl.when(h == 1)
            def _():
                @pl.when(b == 0)
                def _():
                    w_hop(3)

                @pl.when(b == rows)
                def _():
                    w_d_own().wait_recv()
                    for t in range(n_tp):
                        w_d_fwd(t).wait_recv()
                    for i in range(2):
                        w_d_far(i).wait_recv()

            @pl.when(h == 2)
            def _():
                @pl.when((b >= 2) & (b < rows + 2))
                def _():
                    o_hop(b - 2, 3)

                @pl.when((b >= 1) & (b < rows + 1))
                def _():
                    finish(b - 1)

            @pl.when(h == 3)
            def _():
                @pl.when(b == 0)
                def _():
                    w_hop(4)
                    w_x_own().start()
                    w_d_own().start()

                @pl.when(b == rows - 1)
                def _():
                    w_x_own().wait_recv()
                    for t in range(n_tp):
                        w_x_fwd(t).wait_recv()
                    for i in range(2):
                        w_d_far(i).start()

            turn = b * heads + h - (rows * heads + 1)

            @pl.when((turn >= 0) & (turn % 2 == 0) & (turn < 2 * groups - 2) | (turn == 2 * groups))
            def _():
                project_out(jnp.minimum(turn // 2, groups - 1))
            return 0

        lax.fori_loop(0, heads, head, 0)

        @pl.when(b < rows)
        def _():
            l_buf[b] = jnp.transpose(lse_scr[...])[0:8, :]
            for i in range(4):
                p_copy(b, i).start()
        return 0

    lax.fori_loop(0, rows + 3, row, 0)

    for g in range(groups):
        out_copy(g).wait()
    for cpy in outs:
        cpy.wait()

    def sent_g(g, _):
        for i in range(1, n_tp):
            st_copy(g, i).wait_send()
        return 0

    lax.fori_loop(0, groups, sent_g, 0)

    def sent_b(b, _):
        for i in range(6):
            p_copy(b, i).wait_send()
        hop_sent(lambda o: o_all.at[o, b], lambda d, i: z_s.at[b, d * last + i], lambda d, i: z_r.at[b, d * last + i])
        return 0

    lax.fori_loop(0, rows, sent_b, 0)
    hop_sent(lambda o: wf.at[o, js, :], lambda d, i: w_s.at[d * last + i], lambda d, i: w_r.at[d * last + i])
    w_x_own().wait_send()
    w_d_own().wait_send()
    for t in range(n_tp):
        w_y(t).wait_send()
        w_x_fwd(t).wait_send()
        w_d_fwd(t).wait_send()
    for i in range(2):
        w_d_far(i).wait_send()


def solution(mesh):
    n_tp = mesh.shape['tp']

    def local_step(x_chunk, w_query, w_key, w_value, w_out, q_gain, k_gain, post_gain, cache_k, cache_v, prefix_len):
        rows, toks, model = x_chunk.shape
        slots, heads, dim = cache_k.shape[1:]
        width = heads * dim
        n_q = 4 * toks
        positions = prefix_len[:, None] + lax.axis_index('cp') * toks + jnp.arange(toks, dtype=jnp.int32)[None, :]
        inv_freq = ROPE_BASE ** (-(jnp.arange(dim // 2, dtype=F32) * 2.0 / dim))
        angles = positions.astype(F32)[..., None] * inv_freq
        cos, sin = jnp.cos(angles), jnp.sin(angles)
        cos = jnp.concatenate([cos, cos], axis=-1)
        sin = jnp.concatenate([-sin, sin], axis=-1)
        any_ = pl.BlockSpec(memory_space=pl.ANY)
        vm = pl.BlockSpec(memory_space=pltpu.VMEM)
        dma = pltpu.SemaphoreType.DMA
        last = n_tp - 1
        scratch = [
            pltpu.VMEM((rows, toks, model), BF16), pltpu.VMEM((3, model, width), BF16), pltpu.VMEM((n_tp, width, model), BF16),
            pltpu.VMEM((rows, n_q, width), BF16), pltpu.VMEM((rows, toks, width), BF16), pltpu.VMEM((rows, toks, width), BF16),
            pltpu.VMEM((rows, toks, width), BF16), pltpu.VMEM((rows, toks, width), BF16), pltpu.VMEM((rows, toks, width), BF16),
            pltpu.VMEM((rows, 8, toks), F32), pltpu.VMEM((rows, 8, toks), F32), pltpu.VMEM((rows, 8, toks), F32),
            pltpu.VMEM((rows, toks, width), BF16), pltpu.VMEM((rows, 8, toks), F32), pltpu.VMEM((rows, 8, n_q), F32),
            pltpu.VMEM((n_tp, rows, toks, width), BF16), pltpu.VMEM((rows // 2, n_tp, 8, 2 * toks), F32),
            pltpu.VMEM((2, 2, slots * heads, dim), BF16), pltpu.VMEM((1024, 128), F32),
            pltpu.VMEM((heads, slots, dim), BF16), pltpu.VMEM((heads, slots, 2 * dim), BF16),
            pltpu.VMEM((n_q, slots + toks), F32), pltpu.VMEM((n_q, toks), F32), pltpu.VMEM((n_q, 128), F32),
            dma((4 + rows // 2,)), dma((2, 2)), dma((rows // 2 + 2,)), dma((rows // 2, last)), dma((rows // 2, last)),
            dma((rows, 3)), dma((rows, 3)), dma((rows, 6)), dma((rows, 6)), dma((rows, 2 * last)), dma((rows, 2 * last)),
            dma((2 * last + 3 * n_tp + 4,)), dma((2 * last + 3 * n_tp + 4,)),
        ]
        flops = 2 * rows * toks * model * width * 3 + 4 * rows * n_q * slots * width + 2 * rows * toks * model * model
        out, ok, ov = pl.pallas_call(
            functools.partial(step_kernel, n_tp),
            in_specs=[pl.BlockSpec(memory_space=pltpu.SMEM)] + [any_] * 5 + [vm] * 3 + [any_] * 2,
            out_specs=[any_] * 3,
            out_shape=[jax.ShapeDtypeStruct((rows, toks, model), BF16), jax.ShapeDtypeStruct((rows, toks, width), BF16), jax.ShapeDtypeStruct((rows, toks, width), BF16)],
            scratch_shapes=scratch,
            compiler_params=pltpu.CompilerParams(collective_id=0, has_side_effects=True, vmem_limit_bytes=67043328),
            cost_estimate=pl.CostEstimate(flops=flops, bytes_accessed=4 * rows * slots * width, transcendentals=rows * n_q * slots * heads),
            name="step",
        )(prefix_len, x_chunk, w_query, w_key, w_value, w_out, jnp.concatenate([q_gain, k_gain, post_gain]).astype(F32).reshape(1, 2 * width + model),
          cos, sin, cache_k.reshape(rows, slots * heads, dim), cache_v.reshape(rows, slots * heads, dim))
        return out, ok.reshape(rows, toks, heads, dim), ov.reshape(rows, toks, heads, dim)

    x_spec = P('dp', 'cp', None)
    head_spec = P('dp', 'cp', 'tp', None)
    in_specs = (x_spec, P(None, 'tp'), P(None, 'tp'), P(None, 'tp'), P('tp', None), P('tp'), P('tp'), P(None), head_spec, head_spec, P('dp'))
    out_specs = (x_spec, head_spec, head_spec)
    return jax.shard_map(local_step, mesh=mesh, in_specs=in_specs, out_specs=out_specs, check_vma=False)
```

```python
import functools
import jax
import jax.numpy as jnp
from jax import lax
from jax.experimental import pallas as pl
from jax.experimental.pallas import tpu as pltpu
from jax.sharding import PartitionSpec as P

NORM_EPS = 1e-6
ROPE_BASE = 500000.0
MASK_VALUE = -1e30
LOG2E = 1.4426950408889634
MESH = pl.DeviceIdType.MESH
NT = (((1,), (1,)), ((), ()))
F32 = jnp.float32
BF16 = jnp.bfloat16


def split_heads(raw_ref, wide_ref, out_ref, heads, rows):
    step = wide_ref.shape[0]
    per = step // heads

    def body(i, _):
        wide_ref[...] = raw_ref[pl.ds(i * step, step), :].astype(F32)
        for h in range(heads):
            out_ref[h, pl.ds(i * per, per), 0:128] = wide_ref[pl.ds(h, per, stride=heads), :].astype(BF16)
        return 0

    lax.fori_loop(0, rows // step, body, 0)


SCALE = (128 ** -0.5) * LOG2E
TILE = 256


def scores(q, h, kc, bias, k_ref, s_ref, limit):
    n_t = k_ref.shape[1] // TILE
    lane = lax.broadcasted_iota(jnp.int32, (1, TILE), 1)
    s = lax.dot_general(q, kc, NT, preferred_element_type=F32)
    s = jnp.where(bias >= 0, s, MASK_VALUE)
    s_ref[:, n_t * TILE:n_t * TILE + 128] = s
    mx = s
    for j in range(n_t):
        s = lax.dot_general(q, k_ref[h, j * TILE:(j + 1) * TILE, :], NT, preferred_element_type=F32)
        s = jnp.where(lane + j * TILE < limit, s, MASK_VALUE)
        s_ref[:, j * TILE:(j + 1) * TILE] = s
        for u in range(TILE // 128):
            mx = jnp.maximum(mx, s[:, u * 128:(u + 1) * 128])
    return jnp.max(mx, axis=1, keepdims=True) * SCALE


def weigh(top, h, vc, v_ref, s_ref):
    n_t = v_ref.shape[1] // TILE
    acc = None
    for j in range(n_t):
        p = jnp.exp2(s_ref[:, j * TILE:(j + 1) * TILE] * SCALE - top)
        d = jnp.dot(p.astype(BF16), v_ref[h, j * TILE:(j + 1) * TILE, :], preferred_element_type=F32)
        acc = d if acc is None else acc + d
    p = jnp.exp2(s_ref[:, n_t * TILE:n_t * TILE + 128] * SCALE - top)
    return acc + jnp.dot(p.astype(BF16), vc, preferred_element_type=F32)


def attend_head(h, q_ref, kc, vc, k_ref, v_ref, s_ref, limit, bias_ref, lse_ref):
    col = pl.ds(pl.multiple_of(h * 128, 128), 128)
    half = q_ref.shape[0] // 2
    vc = jnp.concatenate([vc, jnp.ones(vc.shape, BF16)], axis=1)
    parts = [slice(r * half, (r + 1) * half) for r in range(2)]
    tops = [scores(q_ref[rs, col], h, kc, bias_ref[rs, :], k_ref, s_ref.at[rs], limit) for rs in parts]
    lane = lax.broadcasted_iota(jnp.int32, (half, 128), 1)
    for rs, top in zip(parts, tops):
        acc = weigh(top, h, vc, v_ref, s_ref.at[rs])
        den = acc[:, 128:]
        q_ref[rs, col] = (acc[:, :128] * (1.0 / den)).astype(BF16)
        lse_ref[rs, :] = jnp.where(lane == h, top + jnp.log2(den), lse_ref[rs, :])


def step_kernel(n_tp, pre_ref, x_hbm, wq_hbm, wk_hbm, wv_hbm, wo_hbm, gain_ref, cos_ref, sin_ref, ck_hbm, cv_hbm,
                out_hbm, ok_hbm, ov_hbm,
                x_v, wqkv, wf, q_buf, kn, vn, rA, rB, rC, lA, lB, lC, c_o, c_l, l_buf, o_all, st,
                raw, wide, k_scr, v_scr, s_scr, bias, lse_scr,
                in_sem, kv_sem, out_sem, st_s, st_r, q_s, q_r, p_s, p_r, z_s, z_r, w_s, w_r):
    rows, toks, model = x_v.shape
    heads, slots = k_scr.shape[0], k_scr.shape[1]
    width = heads * 128
    groups = rows // 2
    gt = 2 * toks
    dp, z, me = lax.axis_index('dp'), lax.axis_index('tp'), lax.axis_index('cp')
    partner = me + 1 - 2 * (me % 2)
    counter = (me + 2) % 4
    diag = 3 - me
    last = n_tp - 1
    piece = wo_hbm.shape[0] // 8

    def remote(src, dst, ss, rs, **dev):
        return pltpu.make_async_remote_copy(src_ref=src, dst_ref=dst, send_sem=ss, recv_sem=rs, device_id=dev, device_id_type=MESH)

    def x_copy(g):
        return pltpu.make_async_copy(x_hbm.at[pl.ds(2 * g, 2)], x_v.at[pl.ds(2 * g, 2)], in_sem.at[4 + g])

    w_copies = [pltpu.make_async_copy(w, wqkv.at[i], in_sem.at[1 + i]) for i, w in enumerate((wq_hbm, wk_hbm, wv_hbm))]
    js = pl.ds(pl.multiple_of((dp * 4 + me) * piece, piece), piece)
    w_local = pltpu.make_async_copy(wo_hbm.at[js, :], wf.at[z, js, :], in_sem.at[0])
    w_copies[0].start()
    x_copy(0).start()
    w_local.start()
    w_copies[1].start()
    w_copies[2].start()
    for g in range(1, groups):
        x_copy(g).start()

    def kv_copies(b):
        par = b % 2
        return (pltpu.make_async_copy(ck_hbm.at[b], raw.at[par, 0], kv_sem.at[par, 0]),
                pltpu.make_async_copy(cv_hbm.at[b], raw.at[par, 1], kv_sem.at[par, 1]))

    for cpy in kv_copies(0):
        cpy.start()

    barrier = pltpu.get_barrier_semaphore()
    for i in range(1, n_tp):
        pl.semaphore_signal(barrier, inc=1, device_id={'tp': (z + i) % n_tp}, device_id_type=MESH)
    pl.semaphore_signal(barrier, inc=1, device_id={'cp': partner}, device_id_type=MESH)
    pl.semaphore_signal(barrier, inc=1, device_id={'cp': counter}, device_id_type=MESH)
    pl.semaphore_signal(barrier, inc=1, device_id={'dp': 1 - dp}, device_id_type=MESH)
    pl.semaphore_wait(barrier, n_tp + 2)

    def hop(buf, send, recv, k, wait_only=False, start=True):
        if k > 1:
            @pl.when(z - (k - 1) >= 0)
            def _():
                remote(buf(z - (k - 1)), buf(z - (k - 1)), send(0, k - 2), recv(0, k - 2), tp=z).wait_recv()

            @pl.when(z + (k - 1) <= last)
            def _():
                remote(buf(z + (k - 1)), buf(z + (k - 1)), send(1, k - 2), recv(1, k - 2), tp=z).wait_recv()
        if k <= last:
            @pl.when((z - (k - 1) >= 0) & (z < last))
            def _():
                remote(buf(z - (k - 1)), buf(z - (k - 1)), send(0, k - 1), recv(0, k - 1), tp=z + 1).start()

            @pl.when((z + (k - 1) <= last) & (z > 0))
            def _():
                remote(buf(z + (k - 1)), buf(z + (k - 1)), send(1, k - 1), recv(1, k - 1), tp=z - 1).start()

    def hop_sent(buf, send, recv):
        for k in range(1, last + 1):
            @pl.when((z - (k - 1) >= 0) & (z < last))
            def _():
                remote(buf(z - (k - 1)), buf(z - (k - 1)), send(0, k - 1), recv(0, k - 1), tp=z).wait_send()

            @pl.when((z + (k - 1) <= last) & (z > 0))
            def _():
                remote(buf(z + (k - 1)), buf(z + (k - 1)), send(1, k - 1), recv(1, k - 1), tp=z).wait_send()

    def w_hop(k):
        hop(lambda o: wf.at[o, js, :], lambda d, i: w_s.at[d * last + i], lambda d, i: w_r.at[d * last + i], k)

    def o_hop(b, k):
        hop(lambda o: o_all.at[o, b], lambda d, i: z_s.at[b, d * last + i], lambda d, i: z_r.at[b, d * last + i], k)

    w_local.wait()
    w_hop(1)

    qi = lax.broadcasted_iota(jnp.int32, (toks, toks), 0)
    ki = lax.broadcasted_iota(jnp.int32, (toks, toks), 1)
    for s, blk in enumerate((me, partner, counter, diag)):
        bias[s * toks:(s + 1) * toks, :] = jnp.where(ki - qi <= (blk - me) * toks, 0.0, -1.0)
    lse_scr[...] = jnp.zeros(lse_scr.shape, F32)
    v_scr[:, :, 128:] = jnp.ones((heads, slots, 128), BF16)

    def st_copy(g, i):
        return remote(st.at[g, 0], st.at[g, i], st_s.at[g, i - 1], st_r.at[g, i - 1], tp=(z + i) % n_tp)

    def q_copy(b, i):
        src = q_buf.at[b, pl.ds(0 if i < 2 else 2 * toks, toks), :]
        dst = q_buf.at[b, pl.ds((i + 1) * toks, toks), :]
        return remote(src, dst, q_s.at[b, i], q_r.at[b, i], cp=counter if i == 1 else partner)

    def project(g):
        x_copy(g).wait()

        @pl.when(g == 0)
        def _():
            w_copies[0].wait()
        xg = x_v[pl.ds(2 * g, 2)].reshape(gt, model)
        cols = pl.ds(pl.multiple_of(g * width, width), width)
        q = jnp.dot(xg, wqkv[0], preferred_element_type=F32)
        s_scr[0:gt, cols] = q

        @pl.when(g == 0)
        def _():
            w_copies[1].wait()
            w_copies[2].wait()
        k = jnp.dot(xg, wqkv[1], preferred_element_type=F32)
        s_scr[gt:2 * gt, cols] = k
        lane = lax.broadcasted_iota(jnp.int32, (gt, 128), 1)
        sq = jnp.sum(q * q, axis=1, keepdims=True)
        sk = jnp.sum(k * k, axis=1, keepdims=True)
        sums = jnp.where(lane == 0, sq, jnp.where(lane == 1, sk, 0.0))
        st[g, 0] = jnp.transpose(sums)[0:8, :]
        v = jnp.dot(xg, wqkv[2], preferred_element_type=F32)
        for i in range(1, n_tp):
            st_copy(g, i).start()
        vn[pl.ds(2 * g, 2)] = v.astype(BF16).reshape(2, toks, width)

    def normalize(g):
        for i in range(1, n_tp):
            st_copy(g, i).wait_recv()
        tot = st[g, 0]
        for i in range(1, n_tp):
            tot = tot + st[g, i]
        inv = jnp.transpose(lax.rsqrt(tot / (width * n_tp) + NORM_EPS))
        for t, (gain, base) in enumerate(((0, 0), (width, gt))):
            for h in range(heads):
                u = s_scr[base:base + gt, pl.ds(pl.multiple_of(g * width + h * 128, 128), 128)]
                u = u * inv[:, t:t + 1] * gain_ref[0:1, gain + h * 128:gain + (h + 1) * 128]
                cos = cos_ref[pl.ds(2 * g, 2)].reshape(gt, 128)
                sin = sin_ref[pl.ds(2 * g, 2)].reshape(gt, 128)
                u = (u * cos + pltpu.roll(u, 64, 1) * sin).astype(BF16).reshape(2, toks, 128)
                if t == 0:
                    q_buf[pl.ds(2 * g, 2), 0:toks, h * 128:(h + 1) * 128] = u
                else:
                    kn[pl.ds(2 * g, 2), :, h * 128:(h + 1) * 128] = u
        for r in range(2):
            q_copy(2 * g + r, 0).start()
            q_copy(2 * g + r, 1).start()

    def front(g, _):
        @pl.when(g < groups)
        def _():
            project(g)

        @pl.when(g > 0)
        def _():
            normalize(g - 1)
        return 0

    lax.fori_loop(0, groups + 1, front, 0)

    n_out = rows * toks * heads
    outs = [pltpu.make_async_copy(raw.at[0, i, pl.ds(0, n_out), :], dst, out_sem.at[groups + i]) for i, dst in enumerate((ok_hbm, ov_hbm))]

    def interleave():
        per = toks * heads

        def one(r, _):
            for i, src in enumerate((kn, vn)):
                for h in range(heads):
                    wide[pl.ds(i * per + h, toks, stride=heads), :] = src[r, :, h * 128:(h + 1) * 128].astype(F32)
            for i in range(2):
                raw[0, i, pl.ds(pl.multiple_of(r * per, per), per), :] = wide[i * per:(i + 1) * per, :].astype(BF16)
            return 0

        lax.fori_loop(0, rows, one, 0)
        for cpy in outs:
            cpy.start()

    nw = 2 * last

    def wslice(d, c):
        return pl.ds(pl.multiple_of((d * 4 + c) * piece, piece), piece)

    def w_send(k, t, ref, **dev):
        return remote(ref, ref, w_s.at[nw + k + t], w_r.at[nw + k + t], **dev)

    def w_y(t):
        return w_send(0, t, wf.at[t, wslice(dp, me), :], cp=counter)

    def w_x_own():
        return w_send(n_tp, 0, wf.at[:, wslice(dp, me), :], dp=1 - dp)

    def w_d_own():
        return w_send(n_tp, 1, wf.at[:, wslice(dp, me), :], cp=partner)

    def w_x_fwd(t):
        return w_send(n_tp + 2, t, wf.at[t, wslice(dp, counter), :], dp=1 - dp)

    def w_d_fwd(t):
        return w_send(2 * n_tp + 2, t, wf.at[t, wslice(dp, counter), :], cp=partner)

    def w_d_far(i):
        return w_send(3 * n_tp + 2, i, wf.at[:, wslice(1 - dp, (me, counter)[i]), :], cp=partner)

    w_hop(2)

    def forward_q(b):
        q_copy(b, 1).wait_recv()
        q_copy(b, 2).start()

    forward_q(0)

    def p_copy(b, i):
        if i < 4:
            s = 1 if i < 2 else 3
            src = (q_buf.at[b, pl.ds(s * toks, toks), :], l_buf.at[b, :, pl.ds(s * toks, toks)])[i % 2]
        else:
            src = (c_o.at[b], c_l.at[b])[i % 2]
        dst = (rA.at[b], lA.at[b], rB.at[b], lB.at[b], rC.at[b], lC.at[b])[i]
        return remote(src, dst, p_s.at[b, i], p_r.at[b, i], cp=partner if i < 4 else counter)

    def blend(parts, dst):
        top = functools.reduce(jnp.maximum, [e for _, e in parts])
        ws = [jnp.exp2(e - top) for _, e in parts]
        den = functools.reduce(jnp.add, ws)
        cols = [jnp.transpose(w / den) for w in ws]
        for h in range(heads):
            hs = slice(h * 128, (h + 1) * 128)
            acc = functools.reduce(jnp.add, [c[:, h:h + 1] * v[:, hs].astype(F32) for c, (v, _) in zip(cols, parts)])
            dst[:, hs] = acc.astype(BF16)
        return top + jnp.log2(den)

    def precombine(b):
        p_copy(b, 2).wait_recv()
        p_copy(b, 3).wait_recv()
        c_l[b] = blend([(q_buf.at[b, pl.ds(2 * toks, toks), :], l_buf[b, :, 2 * toks:3 * toks]), (rB.at[b], lB[b])], c_o.at[b])
        p_copy(b, 4).start()
        p_copy(b, 5).start()

    def finish(b):
        for i in (0, 1, 4, 5):
            p_copy(b, i).wait_recv()
        blend([(q_buf.at[b, pl.ds(0, toks), :], l_buf[b, :, 0:toks]), (rA.at[b], lA[b]), (rC.at[b], lC[b])], o_all.at[z, b])
        o_hop(b, 1)

    def out_copy(g):
        return pltpu.make_async_copy(x_v.at[pl.ds(2 * g, 2)], out_hbm.at[pl.ds(2 * g, 2)], out_sem.at[g])

    def project_out(g):
        o_hop(2 * g, 4)
        o_hop(2 * g + 1, 4)

        def chunk(n, ss):
            cols = pl.ds(pl.multiple_of(n * 512, 512), 512)
            y = None
            for t in range(n_tp):
                d = jnp.dot(o_all[t, pl.ds(2 * g, 2)].reshape(gt, width), wf[t, :, cols], preferred_element_type=F32)
                y = d if y is None else y + d
            s_scr[0:gt, cols] = y
            return ss + jnp.sum(y * y, axis=1, keepdims=True)

        ss = lax.fori_loop(0, model // 512, chunk, jnp.zeros((gt, 1), F32))
        inv = lax.rsqrt(ss / model + NORM_EPS)
        for n in range(model // 512):
            cols = slice(n * 512, (n + 1) * 512)
            y = s_scr[0:gt, cols] * inv * gain_ref[0:1, 2 * width + n * 512:2 * width + (n + 1) * 512]
            y = x_v[pl.ds(2 * g, 2), :, cols].reshape(gt, 512).astype(F32) + y
            x_v[pl.ds(2 * g, 2), :, cols] = y.astype(BF16).reshape(2, toks, 512)
        out_copy(g).start()

    def row(b, _):
        @pl.when(b < rows)
        def _():
            for cpy in kv_copies(b):
                cpy.wait()

            @pl.when(b + 1 < rows)
            def _():
                for cpy in kv_copies(b + 1):
                    cpy.start()
                forward_q(b + 1)

            split_heads(raw.at[b % 2, 0], wide, k_scr, heads, slots * heads)
            split_heads(raw.at[b % 2, 1], wide, v_scr, heads, slots * heads)
            for i in (0, 2):
                q_copy(b, i).wait_recv()
            for i in range(3):
                q_copy(b, i).wait_send()

        limit = pre_ref[jnp.minimum(b, rows - 1)] - me * slots

        def head(h, _):
            @pl.when(b < rows)
            def _():
                col = pl.ds(pl.multiple_of(h * 128, 128), 128)
                attend_head(h, q_buf.at[b], kn[b, :, col], vn[b, :, col], k_scr, v_scr, s_scr, limit, bias, lse_scr)

            @pl.when(h == 0)
            def _():
                @pl.when((b >= 1) & (b < rows + 1))
                def _():
                    precombine(b - 1)

                @pl.when((b >= 1) & (b < 1 + n_tp))
                def _():
                    w_y(b - 1).start()

                @pl.when((b >= 2) & (b < 2 + n_tp))
                def _():
                    w_y(b - 2).wait_recv()
                    w_x_fwd(b - 2).start()
                    w_d_fwd(b - 2).start()

                @pl.when((b >= 3) & (b < rows + 3))
                def _():
                    o_hop(b - 3, 3)

                @pl.when(b == rows + 2)
                def _():
                    interleave()

            @pl.when(h == 1)
            def _():
                @pl.when((b >= 2) & (b < rows + 2))
                def _():
                    o_hop(b - 2, 2)

                @pl.when(b == 0)
                def _():
                    w_hop(3)

                @pl.when(b == rows)
                def _():
                    w_d_own().wait_recv()
                    for t in range(n_tp):
                        w_d_fwd(t).wait_recv()
                    for i in range(2):
                        w_d_far(i).wait_recv()

            @pl.when(h == 2)
            def _():
                @pl.when((b >= 1) & (b < rows + 1))
                def _():
                    finish(b - 1)

            @pl.when(h == 3)
            def _():
                @pl.when(b == 0)
                def _():
                    w_hop(4)
                    w_x_own().start()
                    w_d_own().start()

                @pl.when(b == rows - 1)
                def _():
                    w_x_own().wait_recv()
                    for t in range(n_tp):
                        w_x_fwd(t).wait_recv()
                    for i in range(2):
                        w_d_far(i).start()

            turn = b * heads + h - (rows * heads + 1)

            @pl.when((turn >= 0) & (turn % 2 == 0) & (turn < 2 * groups - 2) | (turn == 2 * groups))
            def _():
                project_out(jnp.minimum(turn // 2, groups - 1))
            return 0

        lax.fori_loop(0, heads, head, 0)

        @pl.when(b < rows)
        def _():
            l_buf[b] = jnp.transpose(lse_scr[...])[0:8, :]
            for i in range(4):
                p_copy(b, i).start()
        return 0

    lax.fori_loop(0, rows + 3, row, 0)

    for g in range(groups):
        out_copy(g).wait()
    for cpy in outs:
        cpy.wait()

    def sent_g(g, _):
        for i in range(1, n_tp):
            st_copy(g, i).wait_send()
        return 0

    lax.fori_loop(0, groups, sent_g, 0)

    def sent_b(b, _):
        for i in range(6):
            p_copy(b, i).wait_send()
        hop_sent(lambda o: o_all.at[o, b], lambda d, i: z_s.at[b, d * last + i], lambda d, i: z_r.at[b, d * last + i])
        return 0

    lax.fori_loop(0, rows, sent_b, 0)
    hop_sent(lambda o: wf.at[o, js, :], lambda d, i: w_s.at[d * last + i], lambda d, i: w_r.at[d * last + i])
    w_x_own().wait_send()
    w_d_own().wait_send()
    for t in range(n_tp):
        w_y(t).wait_send()
        w_x_fwd(t).wait_send()
        w_d_fwd(t).wait_send()
    for i in range(2):
        w_d_far(i).wait_send()


def settle_kernel(n, *refs):
    srcs, dsts, bufs, in_sem, out_sem = refs[:n], refs[n:2 * n], refs[2 * n:3 * n], refs[3 * n], refs[3 * n + 1]
    jobs = []
    for i, (s, d, v) in enumerate(zip(srcs, dsts, bufs)):
        step = s.shape[0] // 8
        for c in range(8):
            rs = pl.ds(c * step, step)
            jobs.append((pltpu.make_async_copy(s.at[rs], v.at[rs], in_sem.at[i, c]), pltpu.make_async_copy(v.at[rs], d.at[rs], out_sem.at[i, c])))
    for a, _ in jobs:
        a.start()
    for a, o in jobs:
        a.wait()
        o.start()
    for _, o in jobs:
        o.wait()


def settle(arrays):
    n = len(arrays)
    any_ = pl.BlockSpec(memory_space=pl.ANY)
    return pl.pallas_call(
        functools.partial(settle_kernel, n), in_specs=[any_] * n, out_specs=[any_] * n,
        out_shape=[jax.ShapeDtypeStruct(a.shape, a.dtype) for a in arrays],
        scratch_shapes=[pltpu.VMEM(a.shape, a.dtype) for a in arrays] + [pltpu.SemaphoreType.DMA((n, 8)), pltpu.SemaphoreType.DMA((n, 8))],
        name="settle")(*arrays)


def solution(mesh):
    n_tp = mesh.shape['tp']

    def local_step(x_chunk, w_query, w_key, w_value, w_out, q_gain, k_gain, post_gain, cache_k, cache_v, prefix_len):
        rows, toks, model = x_chunk.shape
        slots, heads, dim = cache_k.shape[1:]
        width = heads * dim
        n_q = 4 * toks
        positions = prefix_len[:, None] + lax.axis_index('cp') * toks + jnp.arange(toks, dtype=jnp.int32)[None, :]
        inv_freq = ROPE_BASE ** (-(jnp.arange(dim // 2, dtype=F32) * 2.0 / dim))
        angles = positions.astype(F32)[..., None] * inv_freq
        cos, sin = jnp.cos(angles), jnp.sin(angles)
        cos = jnp.concatenate([cos, cos], axis=-1)
        sin = jnp.concatenate([-sin, sin], axis=-1)
        any_ = pl.BlockSpec(memory_space=pl.ANY)
        vm = pl.BlockSpec(memory_space=pltpu.VMEM)
        dma = pltpu.SemaphoreType.DMA
        last = n_tp - 1
        scratch = [
            pltpu.VMEM((rows, toks, model), BF16), pltpu.VMEM((3, model, width), BF16), pltpu.VMEM((n_tp, width, model), BF16),
            pltpu.VMEM((rows, n_q, width), BF16), pltpu.VMEM((rows, toks, width), BF16), pltpu.VMEM((rows, toks, width), BF16),
            pltpu.VMEM((rows, toks, width), BF16), pltpu.VMEM((rows, toks, width), BF16), pltpu.VMEM((rows, toks, width), BF16),
            pltpu.VMEM((rows, 8, toks), F32), pltpu.VMEM((rows, 8, toks), F32), pltpu.VMEM((rows, 8, toks), F32),
            pltpu.VMEM((rows, toks, width), BF16), pltpu.VMEM((rows, 8, toks), F32), pltpu.VMEM((rows, 8, n_q), F32),
            pltpu.VMEM((n_tp, rows, toks, width), BF16), pltpu.VMEM((rows // 2, n_tp, 8, 2 * toks), F32),
            pltpu.VMEM((2, 2, slots * heads, dim), BF16), pltpu.VMEM((1024, 128), F32),
            pltpu.VMEM((heads, slots, dim), BF16), pltpu.VMEM((heads, slots, 2 * dim), BF16),
            pltpu.VMEM((n_q, slots + toks), F32), pltpu.VMEM((n_q, toks), F32), pltpu.VMEM((n_q, 128), F32),
            dma((4 + rows // 2,)), dma((2, 2)), dma((rows // 2 + 2,)), dma((rows // 2, last)), dma((rows // 2, last)),
            dma((rows, 3)), dma((rows, 3)), dma((rows, 6)), dma((rows, 6)), dma((rows, 2 * last)), dma((rows, 2 * last)),
            dma((2 * last + 3 * n_tp + 4,)), dma((2 * last + 3 * n_tp + 4,)),
        ]
        flops = 2 * rows * toks * model * width * 3 + 4 * rows * n_q * slots * width + 2 * rows * toks * model * model
        out, ok, ov = pl.pallas_call(
            functools.partial(step_kernel, n_tp),
            in_specs=[pl.BlockSpec(memory_space=pltpu.SMEM)] + [any_] * 5 + [vm] * 3 + [any_] * 2,
            out_specs=[any_] * 3,
            out_shape=[jax.ShapeDtypeStruct((rows, toks, model), BF16), jax.ShapeDtypeStruct((rows * toks * heads, dim), BF16), jax.ShapeDtypeStruct((rows * toks * heads, dim), BF16)],
            scratch_shapes=scratch,
            compiler_params=pltpu.CompilerParams(collective_id=0, has_side_effects=True, vmem_limit_bytes=67043328),
            cost_estimate=pl.CostEstimate(flops=flops, bytes_accessed=4 * rows * slots * width, transcendentals=rows * n_q * slots * heads),
            name="step",
        )(prefix_len, x_chunk, w_query, w_key, w_value, w_out, jnp.concatenate([q_gain, k_gain, post_gain]).astype(F32).reshape(1, 2 * width + model),
          cos, sin, cache_k.reshape(rows, slots * heads, dim), cache_v.reshape(rows, slots * heads, dim))
        out, ok, ov = settle((out, ok, ov))
        return out, ok.reshape(rows, toks, heads, dim), ov.reshape(rows, toks, heads, dim)

    x_spec = P('dp', 'cp', None)
    head_spec = P('dp', 'cp', 'tp', None)
    in_specs = (x_spec, P(None, 'tp'), P(None, 'tp'), P(None, 'tp'), P('tp', None), P('tp'), P('tp'), P(None), head_spec, head_spec, P('dp'))
    out_specs = (x_spec, head_spec, head_spec)
    return jax.shard_map(local_step, mesh=mesh, in_specs=in_specs, out_specs=out_specs, check_vma=False)
```

```python
import functools
import jax
import jax.numpy as jnp
from jax import lax
from jax.experimental import pallas as pl
from jax.experimental.pallas import tpu as pltpu
from jax.sharding import PartitionSpec as P

NORM_EPS = 1e-6
ROPE_BASE = 500000.0
MASK_VALUE = -1e30
LOG2E = 1.4426950408889634
MESH = pl.DeviceIdType.MESH
NT = (((1,), (1,)), ((), ()))
F32 = jnp.float32
BF16 = jnp.bfloat16


def split_heads(raw_ref, wide_ref, out_ref, heads, rows):
    step = wide_ref.shape[0]
    per = step // heads

    def body(i, _):
        wide_ref[...] = raw_ref[pl.ds(i * step, step), :].astype(F32)
        for h in range(heads):
            out_ref[h, pl.ds(i * per, per), 0:128] = wide_ref[pl.ds(h, per, stride=heads), :].astype(BF16)
        return 0

    lax.fori_loop(0, rows // step, body, 0)


SCALE = (128 ** -0.5) * LOG2E
TILE = 256


def scores(q, h, kc, bias, k_ref, s_ref, limit):
    n_t = k_ref.shape[1] // TILE
    lane = lax.broadcasted_iota(jnp.int32, (1, TILE), 1)
    s = lax.dot_general(q, kc, NT, preferred_element_type=F32)
    s = jnp.where(bias >= 0, s, MASK_VALUE)
    s_ref[:, n_t * TILE:n_t * TILE + 128] = s
    mx = s
    for j in range(n_t):
        s = lax.dot_general(q, k_ref[h, j * TILE:(j + 1) * TILE, :], NT, preferred_element_type=F32)
        s = jnp.where(lane + j * TILE < limit, s, MASK_VALUE)
        s_ref[:, j * TILE:(j + 1) * TILE] = s
        for u in range(TILE // 128):
            mx = jnp.maximum(mx, s[:, u * 128:(u + 1) * 128])
    return jnp.max(mx, axis=1, keepdims=True) * SCALE


def weigh(top, h, vc, v_ref, s_ref):
    n_t = v_ref.shape[1] // TILE
    acc = None
    for j in range(n_t):
        p = jnp.exp2(s_ref[:, j * TILE:(j + 1) * TILE] * SCALE - top)
        d = jnp.dot(p.astype(BF16), v_ref[h, j * TILE:(j + 1) * TILE, :], preferred_element_type=F32)
        acc = d if acc is None else acc + d
    p = jnp.exp2(s_ref[:, n_t * TILE:n_t * TILE + 128] * SCALE - top)
    return acc + jnp.dot(p.astype(BF16), vc, preferred_element_type=F32)


def attend_head(h, q_ref, kc, vc, k_ref, v_ref, s_ref, limit, bias_ref, lse_ref):
    col = pl.ds(pl.multiple_of(h * 128, 128), 128)
    half = q_ref.shape[0] // 2
    vc = jnp.concatenate([vc, jnp.ones(vc.shape, BF16)], axis=1)
    parts = [slice(r * half, (r + 1) * half) for r in range(2)]
    tops = [scores(q_ref[rs, col], h, kc, bias_ref[rs, :], k_ref, s_ref.at[rs], limit) for rs in parts]
    lane = lax.broadcasted_iota(jnp.int32, (half, 128), 1)
    for rs, top in zip(parts, tops):
        acc = weigh(top, h, vc, v_ref, s_ref.at[rs])
        den = acc[:, 128:]
        q_ref[rs, col] = (acc[:, :128] * (1.0 / den)).astype(BF16)
        lse_ref[rs, :] = jnp.where(lane == h % 2, top + jnp.log2(den), lse_ref[rs, :])


def step_kernel(n_tp, pre_ref, x_hbm, wq_hbm, wk_hbm, wv_hbm, wo_hbm, gain_ref, cos_ref, sin_ref, ck_hbm, cv_hbm,
                out_hbm, ok_hbm, ov_hbm,
                x_v, wqkv, wf, q_buf, kn, vn, rA, rB, rC, lA, lB, lC, c_o, c_l, l_buf, o_all, st,
                raw, wide, k_scr, v_scr, s_scr, bias, lse_scr,
                in_sem, kv_sem, out_sem, st_s, st_r, q_s, q_r, p_s, p_r, z_s, z_r, w_s, w_r):
    rows, toks, model = x_v.shape
    heads, slots = k_scr.shape[0], k_scr.shape[1]
    width = heads * 128
    groups = rows // 2
    gt = 2 * toks
    dp, z, me = lax.axis_index('dp'), lax.axis_index('tp'), lax.axis_index('cp')
    partner = me + 1 - 2 * (me % 2)
    counter = (me + 2) % 4
    diag = 3 - me
    last = n_tp - 1
    piece = wo_hbm.shape[0] // 8

    def remote(src, dst, ss, rs, **dev):
        return pltpu.make_async_remote_copy(src_ref=src, dst_ref=dst, send_sem=ss, recv_sem=rs, device_id=dev, device_id_type=MESH)

    def x_copy(g):
        return pltpu.make_async_copy(x_hbm.at[pl.ds(2 * g, 2)], x_v.at[pl.ds(2 * g, 2)], in_sem.at[4 + g])

    w_copies = [pltpu.make_async_copy(w, wqkv.at[i], in_sem.at[1 + i]) for i, w in enumerate((wq_hbm, wk_hbm, wv_hbm))]
    js = pl.ds(pl.multiple_of((dp * 4 + me) * piece, piece), piece)
    w_local = pltpu.make_async_copy(wo_hbm.at[js, :], wf.at[z, js, :], in_sem.at[0])
    w_copies[0].start()
    x_copy(0).start()
    w_local.start()
    w_copies[1].start()
    w_copies[2].start()
    for g in range(1, groups):
        x_copy(g).start()

    def kv_copies(b):
        par = b % 2
        return (pltpu.make_async_copy(ck_hbm.at[b], raw.at[par, 0], kv_sem.at[par, 0]),
                pltpu.make_async_copy(cv_hbm.at[b], raw.at[par, 1], kv_sem.at[par, 1]))

    for cpy in kv_copies(0):
        cpy.start()

    barrier = pltpu.get_barrier_semaphore()
    for i in range(1, n_tp):
        pl.semaphore_signal(barrier, inc=1, device_id={'tp': (z + i) % n_tp}, device_id_type=MESH)
    pl.semaphore_signal(barrier, inc=1, device_id={'cp': partner}, device_id_type=MESH)
    pl.semaphore_signal(barrier, inc=1, device_id={'cp': counter}, device_id_type=MESH)
    pl.semaphore_signal(barrier, inc=1, device_id={'dp': 1 - dp}, device_id_type=MESH)
    pl.semaphore_wait(barrier, n_tp + 2)

    def hop(buf, send, recv, k, wait_only=False, start=True):
        if k > 1:
            @pl.when(z - (k - 1) >= 0)
            def _():
                remote(buf(z - (k - 1)), buf(z - (k - 1)), send(0, k - 2), recv(0, k - 2), tp=z).wait_recv()

            @pl.when(z + (k - 1) <= last)
            def _():
                remote(buf(z + (k - 1)), buf(z + (k - 1)), send(1, k - 2), recv(1, k - 2), tp=z).wait_recv()
        if k <= last:
            @pl.when((z - (k - 1) >= 0) & (z < last))
            def _():
                remote(buf(z - (k - 1)), buf(z - (k - 1)), send(0, k - 1), recv(0, k - 1), tp=z + 1).start()

            @pl.when((z + (k - 1) <= last) & (z > 0))
            def _():
                remote(buf(z + (k - 1)), buf(z + (k - 1)), send(1, k - 1), recv(1, k - 1), tp=z - 1).start()

    def hop_sent(buf, send, recv):
        for k in range(1, last + 1):
            @pl.when((z - (k - 1) >= 0) & (z < last))
            def _():
                remote(buf(z - (k - 1)), buf(z - (k - 1)), send(0, k - 1), recv(0, k - 1), tp=z).wait_send()

            @pl.when((z + (k - 1) <= last) & (z > 0))
            def _():
                remote(buf(z + (k - 1)), buf(z + (k - 1)), send(1, k - 1), recv(1, k - 1), tp=z).wait_send()

    def w_hop(k):
        hop(lambda o: wf.at[o, js, :], lambda d, i: w_s.at[d * last + i], lambda d, i: w_r.at[d * last + i], k)

    def o_copy(u, origin, slot, to):
        ref = o_all.at[origin, u % 2, u // 2]
        return remote(ref, ref, z_s.at[u, slot], z_r.at[u, slot], tp=to)

    sends = [(1, 0), (-1, 1), (2, 2), (-2, 3)]

    def o_send(u):
        for d, slot in sends:
            @pl.when((z + d >= 0) & (z + d <= last))
            def _():
                o_copy(u, z, slot, z + d).start()

    def o_pass(u):
        @pl.when(z == 2)
        def _():
            o_copy(u, 0, 2, z).wait_recv()
            o_copy(u, 0, 4, 3).start()

        @pl.when(z == 1)
        def _():
            o_copy(u, 3, 3, z).wait_recv()
            o_copy(u, 3, 5, 0).start()

    def o_wait(u):
        for d, slot in sends:
            taken = (z == 2) if slot == 2 else (z == 1) if slot == 3 else (z < 0)

            @pl.when((z - d >= 0) & (z - d <= last) & jnp.logical_not(taken))
            def _():
                o_copy(u, z - d, slot, z).wait_recv()

        @pl.when(z == 3)
        def _():
            o_copy(u, 0, 4, z).wait_recv()

        @pl.when(z == 0)
        def _():
            o_copy(u, 3, 5, z).wait_recv()

    def o_sent(u):
        for d, slot in sends:
            @pl.when((z + d >= 0) & (z + d <= last))
            def _():
                o_copy(u, z, slot, z).wait_send()

        @pl.when(z == 2)
        def _():
            o_copy(u, 0, 4, z).wait_send()

        @pl.when(z == 1)
        def _():
            o_copy(u, 3, 5, z).wait_send()

    w_local.wait()
    w_hop(1)

    qi = lax.broadcasted_iota(jnp.int32, (toks, toks), 0)
    ki = lax.broadcasted_iota(jnp.int32, (toks, toks), 1)
    for s, blk in enumerate((me, partner, counter, diag)):
        bias[s * toks:(s + 1) * toks, :] = jnp.where(ki - qi <= (blk - me) * toks, 0.0, -1.0)
    lse_scr[...] = jnp.zeros(lse_scr.shape, F32)
    v_scr[:, :, 128:] = jnp.ones((heads, slots, 128), BF16)

    def st_copy(g, i):
        return remote(st.at[g, 0], st.at[g, i], st_s.at[g, i - 1], st_r.at[g, i - 1], tp=(z + i) % n_tp)

    def q_copy(b, i):
        src = q_buf.at[b, pl.ds(0 if i < 2 else 2 * toks, toks), :]
        dst = q_buf.at[b, pl.ds((i + 1) * toks, toks), :]
        return remote(src, dst, q_s.at[b, i], q_r.at[b, i], cp=counter if i == 1 else partner)

    def project(g):
        x_copy(g).wait()

        @pl.when(g == 0)
        def _():
            w_copies[0].wait()
        xg = x_v[pl.ds(2 * g, 2)].reshape(gt, model)
        cols = pl.ds(pl.multiple_of(g * width, width), width)
        q = jnp.dot(xg, wqkv[0], preferred_element_type=F32)
        s_scr[0:gt, cols] = q

        @pl.when(g == 0)
        def _():
            w_copies[1].wait()
            w_copies[2].wait()
        k = jnp.dot(xg, wqkv[1], preferred_element_type=F32)
        s_scr[gt:2 * gt, cols] = k
        lane = lax.broadcasted_iota(jnp.int32, (gt, 128), 1)
        sq = jnp.sum(q * q, axis=1, keepdims=True)
        sk = jnp.sum(k * k, axis=1, keepdims=True)
        sums = jnp.where(lane == 0, sq, jnp.where(lane == 1, sk, 0.0))
        st[g, 0] = jnp.transpose(sums)[0:8, :]
        v = jnp.dot(xg, wqkv[2], preferred_element_type=F32)
        for i in range(1, n_tp):
            st_copy(g, i).start()
        vn[pl.ds(2 * g, 2)] = v.astype(BF16).reshape(2, toks, width)

    def normalize(g):
        for i in range(1, n_tp):
            st_copy(g, i).wait_recv()
        tot = st[g, 0]
        for i in range(1, n_tp):
            tot = tot + st[g, i]
        inv = jnp.transpose(lax.rsqrt(tot / (width * n_tp) + NORM_EPS))
        for t, (gain, base) in enumerate(((0, 0), (width, gt))):
            for h in range(heads):
                u = s_scr[base:base + gt, pl.ds(pl.multiple_of(g * width + h * 128, 128), 128)]
                u = u * inv[:, t:t + 1] * gain_ref[0:1, gain + h * 128:gain + (h + 1) * 128]
                cos = cos_ref[pl.ds(2 * g, 2)].reshape(gt, 128)
                sin = sin_ref[pl.ds(2 * g, 2)].reshape(gt, 128)
                u = (u * cos + pltpu.roll(u, 64, 1) * sin).astype(BF16).reshape(2, toks, 128)
                if t == 0:
                    q_buf[pl.ds(2 * g, 2), 0:toks, h * 128:(h + 1) * 128] = u
                else:
                    kn[pl.ds(2 * g, 2), :, h * 128:(h + 1) * 128] = u
        for r in range(2):
            q_copy(2 * g + r, 0).start()
            q_copy(2 * g + r, 1).start()

    def front(g, _):
        @pl.when(g < groups)
        def _():
            project(g)

        @pl.when(g > 1)
        def _():
            normalize(g - 2)
        return 0

    lax.fori_loop(0, groups + 2, front, 0)

    n_out = rows * toks * heads
    outs = [pltpu.make_async_copy(raw.at[0, i, pl.ds(0, n_out), :], dst, out_sem.at[groups + i]) for i, dst in enumerate((ok_hbm, ov_hbm))]

    def interleave():
        per = toks * heads

        def one(r, _):
            for i, src in enumerate((kn, vn)):
                for h in range(heads):
                    wide[pl.ds(i * per + h, toks, stride=heads), :] = src[r, :, h * 128:(h + 1) * 128].astype(F32)
            for i in range(2):
                raw[0, i, pl.ds(pl.multiple_of(r * per, per), per), :] = wide[i * per:(i + 1) * per, :].astype(BF16)
            return 0

        lax.fori_loop(0, rows, one, 0)
        for cpy in outs:
            cpy.start()

    nw = 2 * last

    def wslice(d, c):
        return pl.ds(pl.multiple_of((d * 4 + c) * piece, piece), piece)

    def w_send(k, t, ref, **dev):
        return remote(ref, ref, w_s.at[nw + k + t], w_r.at[nw + k + t], **dev)

    def w_y(i):
        half = piece // 2
        return w_send(3 * n_tp + 4, i, wf.at[i // 2, pl.ds(pl.multiple_of((dp * 4 + me) * piece + (i % 2) * half, half), half), :], cp=counter)

    def w_x_own():
        return w_send(n_tp, 0, wf.at[:, wslice(dp, me), :], dp=1 - dp)

    def w_d_own():
        return w_send(n_tp, 1, wf.at[:, wslice(dp, me), :], cp=partner)

    def w_x_fwd(t):
        return w_send(n_tp + 2, t, wf.at[t, wslice(dp, counter), :], dp=1 - dp)

    def w_d_fwd(t):
        return w_send(2 * n_tp + 2, t, wf.at[t, wslice(dp, counter), :], cp=partner)

    def w_d_far(i):
        return w_send(3 * n_tp + 2, i, wf.at[:, wslice(1 - dp, (me, counter)[i]), :], cp=partner)

    w_hop(2)

    def forward_q(b):
        q_copy(b, 1).wait_recv()
        q_copy(b, 2).start()

    forward_q(0)

    half_w = width // 2

    def pair_of(u):
        return pl.ds(pl.multiple_of((u % 2) * half_w, half_w), half_w)

    def p_copy(u, i):
        if i < 4:
            s = 1 if i < 2 else 3
            src = (q_buf.at[u // 2, pl.ds(s * toks, toks), pair_of(u)], l_buf.at[u, :, pl.ds(s * toks, toks)])[i % 2]
        else:
            src = (c_o.at[u], c_l.at[u])[i % 2]
        dst = (rA.at[u], lA.at[u], rB.at[u], lB.at[u], rC.at[u], lC.at[u])[i]
        return remote(src, dst, p_s.at[u, i], p_r.at[u, i], cp=partner if i < 4 else counter)

    def blend(parts, dst):
        top = functools.reduce(jnp.maximum, [e for _, e in parts])
        ws = [jnp.exp2(e - top) for _, e in parts]
        den = functools.reduce(jnp.add, ws)
        cols = [jnp.transpose(w / den) for w in ws]
        for h in range(half_w // 128):
            hs = slice(h * 128, (h + 1) * 128)
            acc = functools.reduce(jnp.add, [c[:, h:h + 1] * v[:, hs].astype(F32) for c, (v, _) in zip(cols, parts)])
            dst[:, hs] = acc.astype(BF16)
        return top + jnp.log2(den)

    def precombine(u):
        p_copy(u, 2).wait_recv()
        p_copy(u, 3).wait_recv()
        c_l[u] = blend([(q_buf.at[u // 2, pl.ds(2 * toks, toks), pair_of(u)], l_buf[u, :, 2 * toks:3 * toks]), (rB.at[u], lB[u])], c_o.at[u])
        p_copy(u, 4).start()
        p_copy(u, 5).start()

    def finish(u):
        for i in (0, 1, 4, 5):
            p_copy(u, i).wait_recv()
        blend([(q_buf.at[u // 2, pl.ds(0, toks), pair_of(u)], l_buf[u, :, 0:toks]), (rA.at[u], lA[u]), (rC.at[u], lC[u])], o_all.at[z, u % 2, u // 2])
        o_send(u)

    def out_copy(g):
        return pltpu.make_async_copy(x_v.at[pl.ds(2 * g, 2)], out_hbm.at[pl.ds(2 * g, 2)], out_sem.at[g])

    def project_out(g):
        for i in range(4):
            o_wait(4 * g + i)

        def chunk(n, ss):
            cols = pl.ds(pl.multiple_of(n * 512, 512), 512)
            y = None
            for t in range(n_tp):
                for i in range(2):
                    d = jnp.dot(o_all[t, i, pl.ds(2 * g, 2)].reshape(gt, half_w), wf[t, i * half_w:(i + 1) * half_w, cols], preferred_element_type=F32)
                    y = d if y is None else y + d
            s_scr[0:gt, cols] = y
            return ss + jnp.sum(y * y, axis=1, keepdims=True)

        ss = lax.fori_loop(0, model // 512, chunk, jnp.zeros((gt, 1), F32))
        inv = lax.rsqrt(ss / model + NORM_EPS)
        for n in range(model // 512):
            cols = slice(n * 512, (n + 1) * 512)
            y = s_scr[0:gt, cols] * inv * gain_ref[0:1, 2 * width + n * 512:2 * width + (n + 1) * 512]
            y = x_v[pl.ds(2 * g, 2), :, cols].reshape(gt, 512).astype(F32) + y
            x_v[pl.ds(2 * g, 2), :, cols] = y.astype(BF16).reshape(2, toks, 512)
        out_copy(g).start()

    def row(b, _):
        @pl.when(b < rows)
        def _():
            for cpy in kv_copies(b):
                cpy.wait()

            @pl.when(b + 1 < rows)
            def _():
                for cpy in kv_copies(b + 1):
                    cpy.start()
                forward_q(b + 1)

            split_heads(raw.at[b % 2, 0], wide, k_scr, heads, slots * heads)
            split_heads(raw.at[b % 2, 1], wide, v_scr, heads, slots * heads)
            for i in (0, 2):
                q_copy(b, i).wait_recv()
            for i in range(3):
                q_copy(b, i).wait_send()

        limit = pre_ref[jnp.minimum(b, rows - 1)] - me * slots

        def head(h, _):
            @pl.when(b < rows)
            def _():
                col = pl.ds(pl.multiple_of(h * 128, 128), 128)
                attend_head(h, q_buf.at[b], kn[b, :, col], vn[b, :, col], k_scr, v_scr, s_scr, limit, bias, lse_scr)

            turn = b * heads + h
            odd = turn % 2 == 1
            n_u = 2 * rows

            even = turn % 2 == 0

            u_send = (turn - 1) // 2

            @pl.when(odd & (u_send < n_u))
            def _():
                l_buf[u_send] = jnp.transpose(lse_scr[...])[0:8, :]
                for i in range(4):
                    p_copy(u_send, i).start()

            u_pre = (turn - 2) // 2

            @pl.when(even & (turn >= 2) & (u_pre < n_u))
            def _():
                precombine(u_pre)

            u_fin = (turn - 5) // 2

            @pl.when(odd & (turn >= 5) & (u_fin < n_u))
            def _():
                finish(u_fin)

            u_far = (turn - 8) // 2

            @pl.when(even & (turn >= 8) & (u_far < n_u))
            def _():
                o_pass(u_far)

            @pl.when((b >= 2) & (b < 2 + n_tp) & even)
            def _():
                w_y((b - 2) * 2 + h // 2).start()

            @pl.when((b >= 3) & (b < 3 + n_tp) & (h == 1))
            def _():
                t = b - 3
                w_y(2 * t).wait_recv()
                w_y(2 * t + 1).wait_recv()
                w_x_fwd(t).start()
                w_d_fwd(t).start()

            @pl.when(turn == 3)
            def _():
                w_hop(3)

            @pl.when(turn == heads + 3)
            def _():
                w_hop(4)
                w_x_own().start()
                w_d_own().start()

            @pl.when(turn == rows * heads - 2)
            def _():
                w_x_own().wait_recv()
                for t in range(n_tp):
                    w_x_fwd(t).wait_recv()
                for i in range(2):
                    w_d_far(i).start()

            @pl.when(turn == rows * heads + 1)
            def _():
                w_d_own().wait_recv()
                for t in range(n_tp):
                    w_d_fwd(t).wait_recv()
                for i in range(2):
                    w_d_far(i).wait_recv()

            @pl.when(turn == rows * heads + 7)
            def _():
                interleave()

            lag = turn - (rows * heads + 1)

            @pl.when((lag == 0) | (lag == 3) | (lag == 4) | (lag == 7))
            def _():
                project_out((lag + 2) // 3)
            return 0

        lax.fori_loop(0, heads, head, 0)
        return 0

    lax.fori_loop(0, rows + 3, row, 0)

    for g in range(groups):
        out_copy(g).wait()
    for cpy in outs:
        cpy.wait()

    def sent_g(g, _):
        for i in range(1, n_tp):
            st_copy(g, i).wait_send()
        return 0

    lax.fori_loop(0, groups, sent_g, 0)

    def sent_b(b, _):
        for i in range(6):
            p_copy(b, i).wait_send()
        o_sent(b)
        return 0

    lax.fori_loop(0, 2 * rows, sent_b, 0)
    hop_sent(lambda o: wf.at[o, js, :], lambda d, i: w_s.at[d * last + i], lambda d, i: w_r.at[d * last + i])
    w_x_own().wait_send()
    w_d_own().wait_send()
    for t in range(n_tp):
        w_y(2 * t).wait_send()
        w_y(2 * t + 1).wait_send()
        w_x_fwd(t).wait_send()
        w_d_fwd(t).wait_send()
    for i in range(2):
        w_d_far(i).wait_send()


def settle_kernel(n, *refs):
    srcs, dsts, bufs, in_sem, out_sem = refs[:n], refs[n:2 * n], refs[2 * n:3 * n], refs[3 * n], refs[3 * n + 1]
    jobs = []
    for i, (s, d, v) in enumerate(zip(srcs, dsts, bufs)):
        step = s.shape[0] // 8
        for c in range(8):
            rs = pl.ds(c * step, step)
            jobs.append((pltpu.make_async_copy(s.at[rs], v.at[rs], in_sem.at[i, c]), pltpu.make_async_copy(v.at[rs], d.at[rs], out_sem.at[i, c])))
    for a, _ in jobs:
        a.start()
    for a, o in jobs:
        a.wait()
        o.start()
    for _, o in jobs:
        o.wait()


def settle(arrays):
    n = len(arrays)
    any_ = pl.BlockSpec(memory_space=pl.ANY)
    return pl.pallas_call(
        functools.partial(settle_kernel, n), in_specs=[any_] * n, out_specs=[any_] * n,
        out_shape=[jax.ShapeDtypeStruct(a.shape, a.dtype) for a in arrays],
        scratch_shapes=[pltpu.VMEM(a.shape, a.dtype) for a in arrays] + [pltpu.SemaphoreType.DMA((n, 8)), pltpu.SemaphoreType.DMA((n, 8))],
        name="settle")(*arrays)


def solution(mesh):
    n_tp = mesh.shape['tp']

    def local_step(x_chunk, w_query, w_key, w_value, w_out, q_gain, k_gain, post_gain, cache_k, cache_v, prefix_len):
        rows, toks, model = x_chunk.shape
        slots, heads, dim = cache_k.shape[1:]
        width = heads * dim
        n_q = 4 * toks
        positions = prefix_len[:, None] + lax.axis_index('cp') * toks + jnp.arange(toks, dtype=jnp.int32)[None, :]
        inv_freq = ROPE_BASE ** (-(jnp.arange(dim // 2, dtype=F32) * 2.0 / dim))
        angles = positions.astype(F32)[..., None] * inv_freq
        cos, sin = jnp.cos(angles), jnp.sin(angles)
        cos = jnp.concatenate([cos, cos], axis=-1)
        sin = jnp.concatenate([-sin, sin], axis=-1)
        any_ = pl.BlockSpec(memory_space=pl.ANY)
        vm = pl.BlockSpec(memory_space=pltpu.VMEM)
        dma = pltpu.SemaphoreType.DMA
        last = n_tp - 1
        scratch = [
            pltpu.VMEM((rows, toks, model), BF16), pltpu.VMEM((3, model, width), BF16), pltpu.VMEM((n_tp, width, model), BF16),
            pltpu.VMEM((rows, n_q, width), BF16), pltpu.VMEM((rows, toks, width), BF16), pltpu.VMEM((rows, toks, width), BF16),
            pltpu.VMEM((2 * rows, toks, width // 2), BF16), pltpu.VMEM((2 * rows, toks, width // 2), BF16), pltpu.VMEM((2 * rows, toks, width // 2), BF16),
            pltpu.VMEM((2 * rows, 8, toks), F32), pltpu.VMEM((2 * rows, 8, toks), F32), pltpu.VMEM((2 * rows, 8, toks), F32),
            pltpu.VMEM((2 * rows, toks, width // 2), BF16), pltpu.VMEM((2 * rows, 8, toks), F32), pltpu.VMEM((2 * rows, 8, n_q), F32),
            pltpu.VMEM((n_tp, 2, rows, toks, width // 2), BF16), pltpu.VMEM((rows // 2, n_tp, 8, 2 * toks), F32),
            pltpu.VMEM((2, 2, slots * heads, dim), BF16), pltpu.VMEM((1024, 128), F32),
            pltpu.VMEM((heads, slots, dim), BF16), pltpu.VMEM((heads, slots, 2 * dim), BF16),
            pltpu.VMEM((n_q, slots + toks), F32), pltpu.VMEM((n_q, toks), F32), pltpu.VMEM((n_q, 128), F32),
            dma((4 + rows // 2,)), dma((2, 2)), dma((rows // 2 + 2,)), dma((rows // 2, last)), dma((rows // 2, last)),
            dma((rows, 3)), dma((rows, 3)), dma((2 * rows, 6)), dma((2 * rows, 6)), dma((2 * rows, 2 * last)), dma((2 * rows, 2 * last)),
            dma((2 * last + 5 * n_tp + 4,)), dma((2 * last + 5 * n_tp + 4,)),
        ]
        flops = 2 * rows * toks * model * width * 3 + 4 * rows * n_q * slots * width + 2 * rows * toks * model * model
        out, ok, ov = pl.pallas_call(
            functools.partial(step_kernel, n_tp),
            in_specs=[pl.BlockSpec(memory_space=pltpu.SMEM)] + [any_] * 5 + [vm] * 3 + [any_] * 2,
            out_specs=[any_] * 3,
            out_shape=[jax.ShapeDtypeStruct((rows, toks, model), BF16), jax.ShapeDtypeStruct((rows * toks * heads, dim), BF16), jax.ShapeDtypeStruct((rows * toks * heads, dim), BF16)],
            scratch_shapes=scratch,
            compiler_params=pltpu.CompilerParams(collective_id=0, has_side_effects=True, vmem_limit_bytes=67043328),
            cost_estimate=pl.CostEstimate(flops=flops, bytes_accessed=4 * rows * slots * width, transcendentals=rows * n_q * slots * heads),
            name="step",
        )(prefix_len, x_chunk, w_query, w_key, w_value, w_out, jnp.concatenate([q_gain, k_gain, post_gain]).astype(F32).reshape(1, 2 * width + model),
          cos, sin, cache_k.reshape(rows, slots * heads, dim), cache_v.reshape(rows, slots * heads, dim))
        out, ok, ov = settle((out, ok, ov))
        return out, ok.reshape(rows, toks, heads, dim), ov.reshape(rows, toks, heads, dim)

    x_spec = P('dp', 'cp', None)
    head_spec = P('dp', 'cp', 'tp', None)
    in_specs = (x_spec, P(None, 'tp'), P(None, 'tp'), P(None, 'tp'), P('tp', None), P('tp'), P('tp'), P(None), head_spec, head_spec, P('dp'))
    out_specs = (x_spec, head_spec, head_spec)
    return jax.shard_map(local_step, mesh=mesh, in_specs=in_specs, out_specs=out_specs, check_vma=False)
```

```python
import functools
import jax
import jax.numpy as jnp
from jax import lax
from jax.experimental import pallas as pl
from jax.experimental.pallas import tpu as pltpu
from jax.sharding import PartitionSpec as P

NORM_EPS = 1e-6
ROPE_BASE = 500000.0
MASK_VALUE = -1e30
LOG2E = 1.4426950408889634
MESH = pl.DeviceIdType.MESH
NT = (((1,), (1,)), ((), ()))
F32 = jnp.float32
BF16 = jnp.bfloat16


def split_quarter(part, raw_ref, wide_ref, outs):
    heads, slots = outs[0].shape[0], outs[0].shape[1]
    step = wide_ref.shape[1]
    per = step // heads
    quarter = slots // 4
    for t, out_ref in enumerate(outs):
        for i in range(quarter // per):
            w = wide_ref.at[t * (quarter // per) + i]
            at = part * quarter + i * per
            for n in range(4):
                rs = pl.ds(pl.multiple_of(at * heads + n * (step // 4), step // 4), step // 4)
                w[n * (step // 4):(n + 1) * (step // 4), :] = raw_ref[t, rs, :].astype(F32)
                yield
            for h in range(heads):
                out_ref[h, pl.ds(pl.multiple_of(at, per), per), :] = w[pl.ds(h, per, stride=heads), :].astype(BF16)
                yield


SCALE = (128 ** -0.5) * LOG2E
TILE = 256


def scores(q, h, kc, bias, k_ref, s_ref, limit, side):
    n_t = k_ref.shape[1] // TILE
    lane = lax.broadcasted_iota(jnp.int32, (1, TILE), 1)
    s = lax.dot_general(q, kc, NT, preferred_element_type=F32)
    s = jnp.where(bias >= 0, s, MASK_VALUE)
    s_ref[:, n_t * TILE:n_t * TILE + 128] = s
    mx = s
    for j in range(n_t):
        s = lax.dot_general(q, k_ref[h, j * TILE:(j + 1) * TILE, :], NT, preferred_element_type=F32)
        s = jnp.where(lane + j * TILE < limit, s, MASK_VALUE)
        s_ref[:, j * TILE:(j + 1) * TILE] = s
        for u in range(TILE // 128):
            mx = jnp.maximum(mx, s[:, u * 128:(u + 1) * 128])
        next(side, None)
    return jnp.max(mx, axis=1, keepdims=True) * SCALE


def weigh(top, h, vc, v_ref, s_ref, side):
    n_t = v_ref.shape[1] // TILE
    acc = None
    for j in range(n_t):
        p = jnp.exp2(s_ref[:, j * TILE:(j + 1) * TILE] * SCALE - top)
        v = v_ref[h, j * TILE:(j + 1) * TILE, :]
        d = jnp.dot(p.astype(BF16), jnp.concatenate([v, jnp.ones(v.shape, BF16)], axis=1), preferred_element_type=F32)
        acc = d if acc is None else acc + d
        next(side, None)
    p = jnp.exp2(s_ref[:, n_t * TILE:n_t * TILE + 128] * SCALE - top)
    return acc + jnp.dot(p.astype(BF16), vc, preferred_element_type=F32)


def attend_head(h, q_ref, kc, vc, k_ref, v_ref, s_ref, limit, bias_ref, lse_ref, side):
    col = pl.ds(pl.multiple_of(h * 128, 128), 128)
    half = q_ref.shape[0] // 2
    vc = jnp.concatenate([vc, jnp.ones(vc.shape, BF16)], axis=1)
    parts = [slice(r * half, (r + 1) * half) for r in range(2)]
    tops = [scores(q_ref[rs, col], h, kc, bias_ref[rs, :], k_ref, s_ref.at[rs], limit, side) for rs in parts]
    lane = lax.broadcasted_iota(jnp.int32, (half, 128), 1)
    for rs, top in zip(parts, tops):
        acc = weigh(top, h, vc, v_ref, s_ref.at[rs], side)
        den = acc[:, 128:]
        q_ref[rs, col] = (acc[:, :128] * (1.0 / den)).astype(BF16)
        lse_ref[rs, :] = jnp.where(lane == h % 2, top + jnp.log2(den), lse_ref[rs, :])


def step_kernel(n_tp, pre_ref, x_hbm, wq_hbm, wk_hbm, wv_hbm, wo_hbm, qg_ref, kg_ref, pg_ref, freq_ref, ck_hbm, cv_hbm,
                out_hbm, ok_hbm, ov_hbm,
                x_v, wqkv, wf, q_buf, kn, vn, rA, rB, rC, lA, lB, lC, c_o, c_l, l_buf, o_all, st,
                raw, cos_ref, sin_ref, wide, k_even, v_even, k_odd, v_odd, s_scr, bias, lse_scr,
                in_sem, kv_sem, out_sem, st_s, st_r, q_s, q_r, p_s, p_r, z_s, z_r, w_s, w_r):
    rows, toks, model = x_v.shape
    heads, slots = k_even.shape[0], k_even.shape[1]
    width = heads * 128
    groups = rows // 2
    gt = 2 * toks
    dp, z, me = lax.axis_index('dp'), lax.axis_index('tp'), lax.axis_index('cp')
    partner = me + 1 - 2 * (me % 2)
    counter = (me + 2) % 4
    diag = 3 - me
    last = n_tp - 1
    piece = wo_hbm.shape[0] // 8

    def remote(src, dst, ss, rs, **dev):
        return pltpu.make_async_remote_copy(src_ref=src, dst_ref=dst, send_sem=ss, recv_sem=rs, device_id=dev, device_id_type=MESH)

    def x_copy(g):
        return pltpu.make_async_copy(x_hbm.at[pl.ds(2 * g, 2)], x_v.at[pl.ds(2 * g, 2)], in_sem.at[4 + g])

    w_copies = [pltpu.make_async_copy(w, wqkv.at[i], in_sem.at[1 + i]) for i, w in enumerate((wq_hbm, wk_hbm, wv_hbm))]
    js = pl.ds(pl.multiple_of((dp * 4 + me) * piece, piece), piece)
    w_local = pltpu.make_async_copy(wo_hbm.at[js, :], wf.at[z, js, :], in_sem.at[0])
    w_copies[0].start()
    x_copy(0).start()
    w_local.start()
    w_copies[1].start()
    w_copies[2].start()
    for g in range(1, groups):
        x_copy(g).start()

    def kv_copies(b):
        par = b % 2
        return (pltpu.make_async_copy(ck_hbm.at[b], raw.at[par, 0], kv_sem.at[par, 0]),
                pltpu.make_async_copy(cv_hbm.at[b], raw.at[par, 1], kv_sem.at[par, 1]))

    for r in range(2):
        for cpy in kv_copies(r):
            cpy.start()

    barrier = pltpu.get_barrier_semaphore()
    for i in range(1, n_tp):
        pl.semaphore_signal(barrier, inc=1, device_id={'tp': (z + i) % n_tp}, device_id_type=MESH)
    pl.semaphore_signal(barrier, inc=1, device_id={'cp': partner}, device_id_type=MESH)
    pl.semaphore_signal(barrier, inc=1, device_id={'cp': counter}, device_id_type=MESH)
    pl.semaphore_signal(barrier, inc=1, device_id={'dp': 1 - dp}, device_id_type=MESH)
    pl.semaphore_wait(barrier, n_tp + 2)

    def hop(buf, send, recv, k, wait_only=False, start=True):
        if k > 1:
            @pl.when(z - (k - 1) >= 0)
            def _():
                remote(buf(z - (k - 1)), buf(z - (k - 1)), send(0, k - 2), recv(0, k - 2), tp=z).wait_recv()

            @pl.when(z + (k - 1) <= last)
            def _():
                remote(buf(z + (k - 1)), buf(z + (k - 1)), send(1, k - 2), recv(1, k - 2), tp=z).wait_recv()
        if k <= last:
            @pl.when((z - (k - 1) >= 0) & (z < last))
            def _():
                remote(buf(z - (k - 1)), buf(z - (k - 1)), send(0, k - 1), recv(0, k - 1), tp=z + 1).start()

            @pl.when((z + (k - 1) <= last) & (z > 0))
            def _():
                remote(buf(z + (k - 1)), buf(z + (k - 1)), send(1, k - 1), recv(1, k - 1), tp=z - 1).start()

    def hop_sent(buf, send, recv):
        for k in range(1, last + 1):
            @pl.when((z - (k - 1) >= 0) & (z < last))
            def _():
                remote(buf(z - (k - 1)), buf(z - (k - 1)), send(0, k - 1), recv(0, k - 1), tp=z).wait_send()

            @pl.when((z + (k - 1) <= last) & (z > 0))
            def _():
                remote(buf(z + (k - 1)), buf(z + (k - 1)), send(1, k - 1), recv(1, k - 1), tp=z).wait_send()

    def w_hop(k):
        hop(lambda o: wf.at[o, js, :], lambda d, i: w_s.at[d * last + i], lambda d, i: w_r.at[d * last + i], k)

    def o_copy(u, origin, slot, to):
        ref = o_all.at[origin, u % 2, u // 2]
        return remote(ref, ref, z_s.at[u, slot], z_r.at[u, slot], tp=to)

    sends = [(1, 0), (-1, 1), (2, 2), (-2, 3)]

    def o_send(u):
        for d, slot in sends:
            @pl.when((z + d >= 0) & (z + d <= last))
            def _():
                o_copy(u, z, slot, z + d).start()

    def o_pass(u):
        @pl.when(z == 2)
        def _():
            o_copy(u, 0, 2, z).wait_recv()
            o_copy(u, 0, 4, 3).start()

        @pl.when(z == 1)
        def _():
            o_copy(u, 3, 3, z).wait_recv()
            o_copy(u, 3, 5, 0).start()

    def o_wait(u):
        for d, slot in sends:
            taken = (z == 2) if slot == 2 else (z == 1) if slot == 3 else (z < 0)

            @pl.when((z - d >= 0) & (z - d <= last) & jnp.logical_not(taken))
            def _():
                o_copy(u, z - d, slot, z).wait_recv()

        @pl.when(z == 3)
        def _():
            o_copy(u, 0, 4, z).wait_recv()

        @pl.when(z == 0)
        def _():
            o_copy(u, 3, 5, z).wait_recv()

    def o_sent(u):
        for d, slot in sends:
            @pl.when((z + d >= 0) & (z + d <= last))
            def _():
                o_copy(u, z, slot, z).wait_send()

        @pl.when(z == 2)
        def _():
            o_copy(u, 0, 4, z).wait_send()

        @pl.when(z == 1)
        def _():
            o_copy(u, 3, 5, z).wait_send()

    w_local.wait()
    w_hop(1)

    qi = lax.broadcasted_iota(jnp.int32, (toks, toks), 0)
    ki = lax.broadcasted_iota(jnp.int32, (toks, toks), 1)
    for s, blk in enumerate((me, partner, counter, diag)):
        bias[s * toks:(s + 1) * toks, :] = jnp.where(ki - qi <= (blk - me) * toks, 0.0, -1.0)
    lse_scr[...] = jnp.zeros(lse_scr.shape, F32)

    low = lax.broadcasted_iota(jnp.int32, (toks, 128), 1) < 64

    def tables(i, _):
        start = jnp.where(low, pre_ref[2 * i], pre_ref[2 * i + 1]) + me * toks
        angle = (start + lax.broadcasted_iota(jnp.int32, (toks, 128), 0)).astype(F32) * freq_ref[0:1, :]
        c, s = jnp.cos(angle), jnp.sin(angle)
        c_far, s_far = pltpu.roll(c, 64, 1), pltpu.roll(s, 64, 1)
        cos_ref[2 * i] = jnp.where(low, c, c_far)
        cos_ref[2 * i + 1] = jnp.where(low, c_far, c)
        sin_ref[2 * i] = jnp.where(low, -s, s_far)
        sin_ref[2 * i + 1] = jnp.where(low, -s_far, s)
        return 0

    lax.fori_loop(0, groups, tables, 0)

    def st_copy(g, i):
        return remote(st.at[g, 0], st.at[g, i], st_s.at[g, i - 1], st_r.at[g, i - 1], tp=(z + i) % n_tp)

    def q_copy(b, i):
        src = q_buf.at[b, pl.ds(0 if i < 2 else 2 * toks, toks), :]
        dst = q_buf.at[b, pl.ds((i + 1) * toks, toks), :]
        return remote(src, dst, q_s.at[b, i], q_r.at[b, i], cp=counter if i == 1 else partner)

    def project(g):
        x_copy(g).wait()

        @pl.when(g == 0)
        def _():
            w_copies[0].wait()
        xg = x_v[pl.ds(2 * g, 2)].reshape(gt, model)
        cols = pl.ds(pl.multiple_of(g * width, width), width)
        q = jnp.dot(xg, wqkv[0], preferred_element_type=F32)
        s_scr[0:gt, cols] = q

        @pl.when(g == 0)
        def _():
            w_copies[1].wait()
            w_copies[2].wait()
        k = jnp.dot(xg, wqkv[1], preferred_element_type=F32)
        s_scr[gt:2 * gt, cols] = k
        lane = lax.broadcasted_iota(jnp.int32, (gt, 128), 1)
        sq = jnp.sum(q * q, axis=1, keepdims=True)
        sk = jnp.sum(k * k, axis=1, keepdims=True)
        sums = jnp.where(lane == 0, sq, jnp.where(lane == 1, sk, 0.0))
        st[g, 0] = jnp.transpose(sums)[0:8, :]
        v = jnp.dot(xg, wqkv[2], preferred_element_type=F32)
        for i in range(1, n_tp):
            st_copy(g, i).start()
        vn[pl.ds(2 * g, 2)] = v.astype(BF16).reshape(2, toks, width)

    def normalize(g):
        for i in range(1, n_tp):
            st_copy(g, i).wait_recv()
        tot = st[g, 0]
        for i in range(1, n_tp):
            tot = tot + st[g, i]
        inv = jnp.transpose(lax.rsqrt(tot / (width * n_tp) + NORM_EPS))
        for t, (gain, base) in enumerate(((qg_ref, 0), (kg_ref, gt))):
            for h in range(heads):
                u = s_scr[base:base + gt, pl.ds(pl.multiple_of(g * width + h * 128, 128), 128)]
                u = u * inv[:, t:t + 1] * gain[0:1, h * 128:(h + 1) * 128]
                cos = cos_ref[pl.ds(2 * g, 2)].reshape(gt, 128)
                sin = sin_ref[pl.ds(2 * g, 2)].reshape(gt, 128)
                u = (u * cos + pltpu.roll(u, 64, 1) * sin).astype(BF16).reshape(2, toks, 128)
                if t == 0:
                    q_buf[pl.ds(2 * g, 2), 0:toks, h * 128:(h + 1) * 128] = u
                else:
                    kn[pl.ds(2 * g, 2), :, h * 128:(h + 1) * 128] = u
        for r in range(2):
            q_copy(2 * g + r, 0).start()
            q_copy(2 * g + r, 1).start()

    def front(g, _):
        @pl.when(g < groups)
        def _():
            project(g)

        @pl.when(g > 1)
        def _():
            normalize(g - 2)
        return 0

    lax.fori_loop(0, groups + 2, front, 0)

    n_out = rows * toks * heads
    outs = [pltpu.make_async_copy(raw.at[0, i, pl.ds(0, n_out), :], dst, out_sem.at[groups + i]) for i, dst in enumerate((ok_hbm, ov_hbm))]

    def interleave():
        per = toks * heads

        def one(r, _):
            for i, src in enumerate((kn, vn)):
                for h in range(heads):
                    wide[0, pl.ds(i * per + h, toks, stride=heads), :] = src[r, :, h * 128:(h + 1) * 128].astype(F32)
            for i in range(2):
                raw[0, i, pl.ds(pl.multiple_of(r * per, per), per), :] = wide[0, i * per:(i + 1) * per, :].astype(BF16)
            return 0

        lax.fori_loop(0, rows, one, 0)
        for cpy in outs:
            cpy.start()

    nw = 2 * last

    def wslice(d, c):
        return pl.ds(pl.multiple_of((d * 4 + c) * piece, piece), piece)

    def w_send(k, t, ref, **dev):
        return remote(ref, ref, w_s.at[nw + k + t], w_r.at[nw + k + t], **dev)

    def w_y(i):
        half = piece // 2
        return w_send(3 * n_tp + 4, i, wf.at[i // 2, pl.ds(pl.multiple_of((dp * 4 + me) * piece + (i % 2) * half, half), half), :], cp=counter)

    def w_x_own():
        return w_send(n_tp, 0, wf.at[:, wslice(dp, me), :], dp=1 - dp)

    def w_d_own():
        return w_send(n_tp, 1, wf.at[:, wslice(dp, me), :], cp=partner)

    def w_x_fwd(t):
        return w_send(n_tp + 2, t, wf.at[t, wslice(dp, counter), :], dp=1 - dp)

    def w_d_fwd(t):
        return w_send(2 * n_tp + 2, t, wf.at[t, wslice(dp, counter), :], cp=partner)

    def w_d_far(i):
        return w_send(3 * n_tp + 2, i, wf.at[:, wslice(1 - dp, (me, counter)[i]), :], cp=partner)

    w_hop(2)

    def forward_q(b):
        q_copy(b, 1).wait_recv()
        q_copy(b, 2).start()

    forward_q(0)

    half_w = width // 2

    def pair_of(u):
        return pl.ds(pl.multiple_of((u % 2) * half_w, half_w), half_w)

    def p_copy(u, i):
        if i < 4:
            s = 1 if i < 2 else 3
            src = (q_buf.at[u // 2, pl.ds(s * toks, toks), pair_of(u)], l_buf.at[u, :, pl.ds(s * toks, toks)])[i % 2]
        else:
            src = (c_o.at[u], c_l.at[u])[i % 2]
        dst = (rA.at[u], lA.at[u], rB.at[u], lB.at[u], rC.at[u], lC.at[u])[i]
        return remote(src, dst, p_s.at[u, i], p_r.at[u, i], cp=partner if i < 4 else counter)

    def blend(parts, dst):
        top = functools.reduce(jnp.maximum, [e for _, e in parts])
        ws = [jnp.exp2(e - top) for _, e in parts]
        den = functools.reduce(jnp.add, ws)
        cols = [jnp.transpose(w / den) for w in ws]
        for h in range(half_w // 128):
            hs = slice(h * 128, (h + 1) * 128)
            acc = functools.reduce(jnp.add, [c[:, h:h + 1] * v[:, hs].astype(F32) for c, (v, _) in zip(cols, parts)])
            dst[:, hs] = acc.astype(BF16)
        return top + jnp.log2(den)

    def precombine(u):
        p_copy(u, 2).wait_recv()
        p_copy(u, 3).wait_recv()
        c_l[u] = blend([(q_buf.at[u // 2, pl.ds(2 * toks, toks), pair_of(u)], l_buf[u, :, 2 * toks:3 * toks]), (rB.at[u], lB[u])], c_o.at[u])
        p_copy(u, 4).start()
        p_copy(u, 5).start()

    def finish(u):
        for i in (0, 1, 4, 5):
            p_copy(u, i).wait_recv()
        blend([(q_buf.at[u // 2, pl.ds(0, toks), pair_of(u)], l_buf[u, :, 0:toks]), (rA.at[u], lA[u]), (rC.at[u], lC[u])], o_all.at[z, u % 2, u // 2])
        o_send(u)

    def out_copy(g):
        return pltpu.make_async_copy(x_v.at[pl.ds(2 * g, 2)], out_hbm.at[pl.ds(2 * g, 2)], out_sem.at[g])

    def project_out(g):
        for i in range(4):
            o_wait(4 * g + i)

        def chunk(n, ss):
            cols = pl.ds(pl.multiple_of(n * 512, 512), 512)
            y = None
            for t in range(n_tp):
                for i in range(2):
                    d = jnp.dot(o_all[t, i, pl.ds(2 * g, 2)].reshape(gt, half_w), wf[t, i * half_w:(i + 1) * half_w, cols], preferred_element_type=F32)
                    y = d if y is None else y + d
            s_scr[0:gt, cols] = y
            return ss + jnp.sum(y * y, axis=1, keepdims=True)

        ss = lax.fori_loop(0, model // 512, chunk, jnp.zeros((gt, 1), F32))
        inv = lax.rsqrt(ss / model + NORM_EPS)
        for n in range(model // 512):
            cols = slice(n * 512, (n + 1) * 512)
            y = s_scr[0:gt, cols] * inv * pg_ref[0:1, n * 512:(n + 1) * 512]
            y = x_v[pl.ds(2 * g, 2), :, cols].reshape(gt, 512).astype(F32) + y
            x_v[pl.ds(2 * g, 2), :, cols] = y.astype(BF16).reshape(2, toks, 512)
        out_copy(g).start()

    for cpy in kv_copies(0):
        cpy.wait()

    def first_row(h, _):
        for _ in split_quarter(h, raw.at[0], wide, (k_even, v_even)):
            pass
        return 0

    lax.fori_loop(0, heads, first_row, 0)

    def row(b, _):
        @pl.when(b < rows)
        def _():
            @pl.when(b + 1 < rows)
            def _():
                for cpy in kv_copies(b + 1):
                    cpy.wait()
                forward_q(b + 1)

            @pl.when(b + 2 < rows)
            def _():
                for cpy in kv_copies(b + 2):
                    cpy.start()

            for i in (0, 2):
                q_copy(b, i).wait_recv()
            for i in range(3):
                q_copy(b, i).wait_send()

        limit = pre_ref[jnp.minimum(b, rows - 1)] - me * slots

        def head(h, _):
            col = pl.ds(pl.multiple_of(h * 128, 128), 128)
            for parity, now, nxt in ((0, (k_even, v_even), (k_odd, v_odd)), (1, (k_odd, v_odd), (k_even, v_even))):
                @pl.when((b < rows) & (b % 2 == parity))
                def _():
                    side = split_quarter(h, raw.at[1 - parity], wide, nxt)
                    attend_head(h, q_buf.at[b], kn[b, :, col], vn[b, :, col], now[0], now[1], s_scr, limit, bias, lse_scr, side)
                    for _ in side:
                        pass

            turn = b * heads + h
            odd = turn % 2 == 1
            n_u = 2 * rows

            even = turn % 2 == 0

            u_send = (turn - 1) // 2

            @pl.when(odd & (u_send < n_u))
            def _():
                l_buf[u_send] = jnp.transpose(lse_scr[...])[0:8, :]
                for i in range(4):
                    p_copy(u_send, i).start()

            u_pre = (turn - 2) // 2

            @pl.when(even & (turn >= 2) & (u_pre < n_u))
            def _():
                precombine(u_pre)

            u_fin = (turn - 5) // 2

            @pl.when(odd & (turn >= 5) & (u_fin < n_u))
            def _():
                finish(u_fin)

            u_far = (turn - 8) // 2

            @pl.when(even & (turn >= 8) & (u_far < n_u))
            def _():
                o_pass(u_far)

            @pl.when((b >= 2) & (b < 2 + n_tp) & even)
            def _():
                w_y((b - 2) * 2 + h // 2).start()

            @pl.when((b >= 3) & (b < 3 + n_tp) & (h == 1))
            def _():
                t = b - 3
                w_y(2 * t).wait_recv()
                w_y(2 * t + 1).wait_recv()
                w_x_fwd(t).start()
                w_d_fwd(t).start()

            @pl.when(turn == 3)
            def _():
                w_hop(3)

            @pl.when(turn == heads + 3)
            def _():
                w_hop(4)
                w_x_own().start()
                w_d_own().start()

            @pl.when(turn == rows * heads - 2)
            def _():
                w_x_own().wait_recv()
                for t in range(n_tp):
                    w_x_fwd(t).wait_recv()
                for i in range(2):
                    w_d_far(i).start()

            @pl.when(turn == rows * heads + 1)
            def _():
                w_d_own().wait_recv()
                for t in range(n_tp):
                    w_d_fwd(t).wait_recv()
                for i in range(2):
                    w_d_far(i).wait_recv()

            @pl.when(turn == rows * heads + 7)
            def _():
                interleave()

            lag = turn - (rows * heads + 1)

            @pl.when((lag == 0) | (lag == 3) | (lag == 4) | (lag == 7))
            def _():
                project_out((lag + 2) // 3)
            return 0

        lax.fori_loop(0, heads, head, 0)
        return 0

    lax.fori_loop(0, rows + 3, row, 0)

    for g in range(groups):
        out_copy(g).wait()
    for cpy in outs:
        cpy.wait()

    def sent_g(g, _):
        for i in range(1, n_tp):
            st_copy(g, i).wait_send()
        return 0

    lax.fori_loop(0, groups, sent_g, 0)

    def sent_b(b, _):
        for i in range(6):
            p_copy(b, i).wait_send()
        o_sent(b)
        return 0

    lax.fori_loop(0, 2 * rows, sent_b, 0)
    hop_sent(lambda o: wf.at[o, js, :], lambda d, i: w_s.at[d * last + i], lambda d, i: w_r.at[d * last + i])
    w_x_own().wait_send()
    w_d_own().wait_send()
    for t in range(n_tp):
        w_y(2 * t).wait_send()
        w_y(2 * t + 1).wait_send()
        w_x_fwd(t).wait_send()
        w_d_fwd(t).wait_send()
    for i in range(2):
        w_d_far(i).wait_send()


def settle_kernel(n, *refs):
    srcs, dsts, bufs, in_sem, out_sem = refs[:n], refs[n:2 * n], refs[2 * n:3 * n], refs[3 * n], refs[3 * n + 1]
    jobs = []
    for i, (s, d, v) in enumerate(zip(srcs, dsts, bufs)):
        step = s.shape[0] // 8
        for c in range(8):
            rs = pl.ds(c * step, step)
            jobs.append((pltpu.make_async_copy(s.at[rs], v.at[rs], in_sem.at[i, c]), pltpu.make_async_copy(v.at[rs], d.at[rs], out_sem.at[i, c])))
    for a, _ in jobs:
        a.start()
    for a, o in jobs:
        a.wait()
        o.start()
    for _, o in jobs:
        o.wait()


def settle(arrays):
    n = len(arrays)
    any_ = pl.BlockSpec(memory_space=pl.ANY)
    return pl.pallas_call(
        functools.partial(settle_kernel, n), in_specs=[any_] * n, out_specs=[any_] * n,
        out_shape=[jax.ShapeDtypeStruct(a.shape, a.dtype) for a in arrays],
        scratch_shapes=[pltpu.VMEM(a.shape, a.dtype) for a in arrays] + [pltpu.SemaphoreType.DMA((n, 8)), pltpu.SemaphoreType.DMA((n, 8))],
        name="settle")(*arrays)


def solution(mesh):
    n_tp = mesh.shape['tp']

    def local_step(x_chunk, w_query, w_key, w_value, w_out, q_gain, k_gain, post_gain, cache_k, cache_v, prefix_len):
        rows, toks, model = x_chunk.shape
        slots, heads, dim = cache_k.shape[1:]
        width = heads * dim
        n_q = 4 * toks
        inv_freq = ROPE_BASE ** (-(jnp.arange(dim // 2, dtype=F32) * 2.0 / dim))
        freq = jnp.concatenate([inv_freq, inv_freq]).reshape(1, dim)
        any_ = pl.BlockSpec(memory_space=pl.ANY)
        vm = pl.BlockSpec(memory_space=pltpu.VMEM)
        dma = pltpu.SemaphoreType.DMA
        last = n_tp - 1
        scratch = [
            pltpu.VMEM((rows, toks, model), BF16), pltpu.VMEM((3, model, width), BF16), pltpu.VMEM((n_tp, width, model), BF16),
            pltpu.VMEM((rows, n_q, width), BF16), pltpu.VMEM((rows, toks, width), BF16), pltpu.VMEM((rows, toks, width), BF16),
            pltpu.VMEM((2 * rows, toks, width // 2), BF16), pltpu.VMEM((2 * rows, toks, width // 2), BF16), pltpu.VMEM((2 * rows, toks, width // 2), BF16),
            pltpu.VMEM((2 * rows, 8, toks), F32), pltpu.VMEM((2 * rows, 8, toks), F32), pltpu.VMEM((2 * rows, 8, toks), F32),
            pltpu.VMEM((2 * rows, toks, width // 2), BF16), pltpu.VMEM((2 * rows, 8, toks), F32), pltpu.VMEM((2 * rows, 8, n_q), F32),
            pltpu.VMEM((n_tp, 2, rows, toks, width // 2), BF16), pltpu.VMEM((rows // 2, n_tp, 8, 2 * toks), F32),
            pltpu.VMEM((2, 2, slots * heads, dim), BF16), pltpu.VMEM((rows, toks, dim), F32), pltpu.VMEM((rows, toks, dim), F32), pltpu.VMEM((4, 1024, 128), F32),
            pltpu.VMEM((heads, slots, dim), BF16), pltpu.VMEM((heads, slots, dim), BF16), pltpu.VMEM((heads, slots, dim), BF16), pltpu.VMEM((heads, slots, dim), BF16),
            pltpu.VMEM((n_q, slots + toks), F32), pltpu.VMEM((n_q, toks), F32), pltpu.VMEM((n_q, 128), F32),
            dma((4 + rows // 2,)), dma((2, 2)), dma((rows // 2 + 2,)), dma((rows // 2, last)), dma((rows // 2, last)),
            dma((rows, 3)), dma((rows, 3)), dma((2 * rows, 6)), dma((2 * rows, 6)), dma((2 * rows, 2 * last)), dma((2 * rows, 2 * last)),
            dma((2 * last + 5 * n_tp + 4,)), dma((2 * last + 5 * n_tp + 4,)),
        ]
        flops = 2 * rows * toks * model * width * 3 + 4 * rows * n_q * slots * width + 2 * rows * toks * model * model
        out, ok, ov = pl.pallas_call(
            functools.partial(step_kernel, n_tp),
            in_specs=[pl.BlockSpec(memory_space=pltpu.SMEM)] + [any_] * 5 + [vm] * 4 + [any_] * 2,
            out_specs=[any_] * 3,
            out_shape=[jax.ShapeDtypeStruct((rows, toks, model), BF16), jax.ShapeDtypeStruct((rows * toks * heads, dim), BF16), jax.ShapeDtypeStruct((rows * toks * heads, dim), BF16)],
            scratch_shapes=scratch,
            compiler_params=pltpu.CompilerParams(collective_id=0, has_side_effects=True, vmem_limit_bytes=67043328),
            cost_estimate=pl.CostEstimate(flops=flops, bytes_accessed=4 * rows * slots * width, transcendentals=rows * n_q * slots * heads),
            name="step",
        )(prefix_len, x_chunk, w_query, w_key, w_value, w_out, q_gain.astype(F32).reshape(1, width), k_gain.astype(F32).reshape(1, width), post_gain.astype(F32).reshape(1, model), freq,
          cache_k.reshape(rows, slots * heads, dim), cache_v.reshape(rows, slots * heads, dim))
        out, ok, ov = settle((out, ok, ov))
        return out, ok.reshape(rows, toks, heads, dim), ov.reshape(rows, toks, heads, dim)

    x_spec = P('dp', 'cp', None)
    head_spec = P('dp', 'cp', 'tp', None)
    in_specs = (x_spec, P(None, 'tp'), P(None, 'tp'), P(None, 'tp'), P('tp', None), P('tp'), P('tp'), P(None), head_spec, head_spec, P('dp'))
    out_specs = (x_spec, head_spec, head_spec)
    return jax.shard_map(local_step, mesh=mesh, in_specs=in_specs, out_specs=out_specs, check_vma=False)
```
